32 devices in a mesh: wide: 16 (over z, x, core), narrow: 2 (over y).
Axes of the slice: x: 2, y: 2, z: 4, core: 2. Of those that a mesh axis runs over, the one named last changes fastest.
Arguments:
- design: float32 [192, 96, 384], P('wide', 'narrow'), may hold values from 0 to 1
- passive: int32 [192, 96, 384], P('wide', 'narrow'), may hold values 0 or 1
- displacement: float32 [3, 3, 64, 32, 128], P(None, None, 'wide', 'narrow'), may hold values from -6 to 6
- support: int32 [64, 32, 128], P('wide', 'narrow'), may hold values 0 or 1
- loading: int32 [64, 32, 128], P('wide', 'narrow'), may hold values 0 or 1
Outputs:
- residual: float32 [3, 3, 64, 32, 128], P(None, None, 'wide', 'narrow')
- compliance: float32 [3], replicated
- sensitivity: float32 [192, 96, 384], P('wide', 'narrow')
The draws below stay inside these ranges and needn't reach their ends.
All inputs are finite; a program needn't handle non-finite values. No bound on the sum of `passive` or of `support` or of `loading` on one device may be relied on, other than what follows from the above.
Results may differ from the reference program's by a relative error of at most 0.0001.
Values sent between devices are 32-bit elements; how exact they have to be, the bound alone decides.
No kernel may reach another device: no remote copies, remote signals or barrier semaphores. Data moves between devices by JAX's collectives and lax.ppermute only.
A program may use at most 64 MiB of HBM per device.

```python
import math
import jax
import jax.numpy as jnp
import numpy as np
from jax import lax

ELEMENTS_THIRD = 128
RAD = 3
ELEMENTS_FIRST = 64
ELEMENTS_SECOND = 32
NX = 192
NY = 96
VOXELS_THIRD = 384


def plant(values, stream_key, least, largest):
    shape = values.shape
    index_at = [jax.random.randint(jax.random.fold_in(stream_key, axis), (), 0, shape[axis]) for axis in range(len(shape))]
    values = values.at[tuple(index_at)].set(least)
    longest = shape.index(max(shape))
    index_at[longest] = (index_at[longest] + 1) % shape[longest]
    return values.at[tuple(index_at)].set(largest)


def levels(key, shape, cuts, low, largest):
    def one(axis_at, shards_of):
        steps = jax.random.uniform(jax.random.fold_in(jax.random.fold_in(key, 6), axis_at), (shards_of,), jnp.float32, low / len(cuts), largest / len(cuts))
        return jnp.repeat(jnp.exp(steps), shape[axis_at] // shards_of).reshape((-1,) + (1,) * (len(shape) - axis_at - 1))

    factor_of = one(*cuts[0])
    for cut in cuts[1:]:
        factor_of = factor_of * one(*cut)
    return factor_of


def noise(own_key, shape, scale, most, split=(), held_as=jnp.bfloat16):
    gain = levels(own_key, shape, split, -0.22, 0.18) if split else 1.0
    entries = jax.random.normal(own_key, shape, jnp.float32) * scale * gain
    return jnp.minimum(jnp.maximum(entries, -most), most).astype(held_as)


def setup_inputs(seed: int = 0) -> dict:
    seeds = jax.random.split(jax.random.key(seed), 6)
    return {
        "design": jnp.clip(1.0 * jax.random.uniform(seeds[0], (NX, NY, VOXELS_THIRD), jnp.float32) ** levels(seeds[0], (NX, NY, VOXELS_THIRD), ((0, 16), (1, 2)), -0.2, 0.2), 0.0, 1.0),
        "passive": plant((jax.random.randint(seeds[1], (NX, NY, VOXELS_THIRD), 0, 8) < 1).astype(jnp.int32), jax.random.fold_in(seeds[1], 1), 0, 1),
        "displacement": noise(seeds[2], (3, 3, ELEMENTS_FIRST, ELEMENTS_SECOND, ELEMENTS_THIRD), 1.0, 6.0, ((2, 16), (3, 2)), jnp.float32),
        "support": plant((jax.random.randint(seeds[3], (ELEMENTS_FIRST, ELEMENTS_SECOND, ELEMENTS_THIRD), 0, 16) < 1).astype(jnp.int32), jax.random.fold_in(seeds[3], 1), 0, 1),
        "loading": plant((jax.random.randint(seeds[4], (ELEMENTS_FIRST, ELEMENTS_SECOND, ELEMENTS_THIRD), 0, 16) < 1).astype(jnp.int32), jax.random.fold_in(seeds[4], 1), 0, 1),
    }


sharpness = 8.0
thresholds = (0.7, 0.5, 0.3)
stiff_floor = 0.001
load_force = 4.0
poisson = 0.3

def element_matrix():
    inv_root = 1.0 / np.sqrt(3.0)
    elastic_scale = 1.0 / ((1.0 + poisson) * (1.0 - 2.0 * poisson))
    elastic = np.zeros((6, 6))
    for row_i in range(3):
        for col_j in range(3):
            elastic[row_i, col_j] = poisson
        elastic[row_i, row_i] = 1.0 - poisson
    for row_i in range(3, 6):
        elastic[row_i, row_i] = 0.5 - poisson
    elastic = elastic * elastic_scale
    corner_signs = [(2 * (corner // 4) - 1, 2 * (corner // 2 % 2) - 1, 2 * (corner % 2) - 1) for corner in range(8)]
    stiffness = np.zeros((24, 24))
    for gauss_a in (-inv_root, inv_root):
        for gauss_b in (-inv_root, inv_root):
            for gauss_c in (-inv_root, inv_root):
                gauss_point = (gauss_a, gauss_b, gauss_c)
                derivs = np.zeros((8, 3))
                for corner in range(8):
                    for along in range(3):
                        slope_value = corner_signs[corner][along] / 8.0
                        for second in range(3):
                            if second != along:
                                slope_value = slope_value * (1.0 + corner_signs[corner][second] * gauss_point[second])
                        derivs[corner, along] = 2.0 * slope_value
                strain = np.zeros((6, 24))
                for corner in range(8):
                    column = 3 * corner
                    strain[0, column] = derivs[corner, 0]
                    strain[1, column + 1] = derivs[corner, 1]
                    strain[2, column + 2] = derivs[corner, 2]
                    strain[3, column] = derivs[corner, 1]
                    strain[3, column + 1] = derivs[corner, 0]
                    strain[4, column + 1] = derivs[corner, 2]
                    strain[4, column + 2] = derivs[corner, 1]
                    strain[5, column] = derivs[corner, 2]
                    strain[5, column + 2] = derivs[corner, 0]
                stiffness = stiffness + strain.T @ elastic @ strain * 0.125
    return stiffness.astype(np.float32)

def blur_axis(padded, axis_dim, length):
    summed = float(1 - RAD + RAD) * lax.slice_in_dim(padded, 0, length, axis=axis_dim)
    for offset in range(1, 2 * RAD + 1):
        summed = summed + float(RAD + 1 - abs(offset - RAD)) * lax.slice_in_dim(padded, offset, offset + length, axis=axis_dim)
    return summed

def edge_weights(start_index, amount, extent):
    places = start_index + jnp.arange(amount, dtype=jnp.int32)
    summed = jnp.zeros((amount,), jnp.float32)
    for offset in range(-RAD, RAD + 1):
        inside = ((places + offset >= 0) & (places + offset < extent)).astype(jnp.float32)
        summed = summed + float(RAD + 1 - abs(offset)) * inside
    return summed

def smooth_field(source):
    padded = jnp.pad(source, RAD)
    rowwise = blur_axis(padded, 0, source.shape[0])
    colwise = blur_axis(rowwise, 1, source.shape[1])
    return blur_axis(colwise, 2, source.shape[2])

def project(blurred, threshold):
    low_end = float(math.tanh(sharpness * threshold))
    denominator = low_end + float(math.tanh(sharpness * (1.0 - threshold)))
    steep_part = jnp.tanh(sharpness * (blurred - threshold))
    return ((low_end + steep_part) / denominator, sharpness * (1.0 - steep_part * steep_part) / denominator)

def depth_averaging(fine_len, coarse_len):
    rows_index = jnp.arange(fine_len, dtype=jnp.int32)[:, None] // 3
    cols_index = jnp.arange(coarse_len, dtype=jnp.int32)[None, :]
    return (rows_index == cols_index).astype(jnp.float32)

def aggregate(fine_stiff, coarse_averaging, count_x, count_y):
    merged = jnp.dot(fine_stiff.reshape(-1, fine_stiff.shape[2]), coarse_averaging, precision=lax.Precision.HIGHEST)
    merged = merged.reshape(count_x, 3, count_y, 3, coarse_averaging.shape[1])
    return lax.optimization_barrier(jnp.sum(merged, axis=(1, 3))) / 27.0

def spread(coarse, coarse_averaging):
    count_x, count_y, count_z = coarse.shape
    deepened = jnp.dot(coarse.reshape(-1, count_z), coarse_averaging.T, precision=lax.Precision.HIGHEST)
    deepened = deepened.reshape(count_x, 1, count_y, 1, coarse_averaging.shape[0])
    return jnp.broadcast_to(deepened, (count_x, 3, count_y, 3, coarse_averaging.shape[0])).reshape(3 * count_x, 3 * count_y, coarse_averaging.shape[0])

def element_contributions(nodal_values, moduli, count_x, count_y, count_z, operator_matrix):
    batch = nodal_values.shape[0]
    corners = []
    for corner in range(8):
        along_x, along_y, along_z = (corner // 4, corner // 2 % 2, corner % 2)
        corners.append(nodal_values[:, :, along_x:along_x + count_x, along_y:along_y + count_y, along_z:along_z + count_z])
    stacked = jnp.stack(corners, axis=1).reshape(batch, 24, count_x, count_y, count_z)
    product = jnp.einsum('ij,bjxyz->bixyz', operator_matrix, stacked, precision=lax.Precision.HIGHEST)
    strain_energy = lax.optimization_barrier(jnp.sum(stacked * product, axis=1))
    return (strain_energy, moduli[:, None] * product)

def gather_global(external_loads, count_x, count_y, count_z):
    summed = jnp.zeros((external_loads.shape[0], 3, count_x + 1, count_y + 1, count_z + 1), jnp.float32)
    for corner in range(8):
        along_x, along_y, along_z = (corner // 4, corner // 2 % 2, corner % 2)
        summed = summed.at[:, :, along_x:along_x + count_x, along_y:along_y + count_y, along_z:along_z + count_z].add(external_loads[:, 3 * corner:3 * corner + 3])
    return summed

def reference(design, passive, displacement, support, loading):
    solid_mask = 1.0 - passive.astype(jnp.float32)
    freedom = 1.0 - support.astype(jnp.float32)
    load_values = load_force * loading.astype(jnp.float32)
    weights = edge_weights(0, NX, NX)[:, None, None] * edge_weights(0, NY, NY)[None, :, None] * edge_weights(0, VOXELS_THIRD, VOXELS_THIRD)[None, None, :]
    blurred = smooth_field(design) / weights
    coarse_averaging = depth_averaging(VOXELS_THIRD, ELEMENTS_THIRD)
    operator_matrix = jnp.asarray(element_matrix(), dtype=jnp.float32)
    zeros_field = jnp.zeros_like(load_values)
    applied = jnp.stack([zeros_field, zeros_field, -load_values])
    residuals = []
    compliances = []
    gradient = jnp.zeros_like(design)
    for level_index in range(3):
        density, slope_term = project(blurred, thresholds[level_index])
        density = density * solid_mask
        young_modulus = aggregate(stiff_floor + (1.0 - stiff_floor) * density ** 3, coarse_averaging, ELEMENTS_FIRST, ELEMENTS_SECOND)
        masked_moves = displacement[level_index] * freedom
        nodal_values = jnp.pad(masked_moves, ((0, 0), (0, 1), (0, 1), (0, 1)))[None]
        strain_energy, external_loads = element_contributions(nodal_values, young_modulus[None], ELEMENTS_FIRST, ELEMENTS_SECOND, ELEMENTS_THIRD, operator_matrix)
        global_gathered = gather_global(external_loads, ELEMENTS_FIRST, ELEMENTS_SECOND, ELEMENTS_THIRD)[0, :, :ELEMENTS_FIRST, :ELEMENTS_SECOND, :ELEMENTS_THIRD]
        residuals.append((applied - global_gathered) * freedom)
        compliance = jnp.sum(young_modulus * strain_energy[0])
        compliances.append(compliance)
        gradient = gradient - 3.0 * (1.0 - stiff_floor) / 27.0 * density ** 2 * spread(strain_energy[0] / compliance, coarse_averaging) * slope_term * solid_mask
    sensitivity = smooth_field(gradient / weights)
    return (jnp.stack(residuals), jnp.stack(compliances), sensitivity)
```

```python
import functools
import math

import jax
import jax.numpy as jnp
import numpy as np
from jax import lax
from jax.experimental import pallas as pl
from jax.experimental.pallas import tpu as pltpu
from jax.sharding import PartitionSpec as P

RAD = 3
sharpness = 8.0
thresholds = (0.7, 0.5, 0.3)
stiff_floor = 0.001
load_force = 4.0
poisson = 0.3
LANES = 128
REACH = 2 * RAD


def element_matrix():
    inv_root = 1.0 / np.sqrt(3.0)
    elastic_scale = 1.0 / ((1.0 + poisson) * (1.0 - 2.0 * poisson))
    elastic = np.zeros((6, 6))
    for row_i in range(3):
        for col_j in range(3):
            elastic[row_i, col_j] = poisson
        elastic[row_i, row_i] = 1.0 - poisson
    for row_i in range(3, 6):
        elastic[row_i, row_i] = 0.5 - poisson
    elastic = elastic * elastic_scale
    corner_signs = [
        (2 * (corner // 4) - 1, 2 * (corner // 2 % 2) - 1, 2 * (corner % 2) - 1)
        for corner in range(8)
    ]
    stiffness = np.zeros((24, 24))
    for gauss_a in (-inv_root, inv_root):
        for gauss_b in (-inv_root, inv_root):
            for gauss_c in (-inv_root, inv_root):
                gauss_point = (gauss_a, gauss_b, gauss_c)
                derivs = np.zeros((8, 3))
                for corner in range(8):
                    for along in range(3):
                        slope_value = corner_signs[corner][along] / 8.0
                        for second in range(3):
                            if second != along:
                                slope_value = slope_value * (
                                    1.0 + corner_signs[corner][second] * gauss_point[second]
                                )
                        derivs[corner, along] = 2.0 * slope_value
                strain = np.zeros((6, 24))
                for corner in range(8):
                    column = 3 * corner
                    strain[0, column] = derivs[corner, 0]
                    strain[1, column + 1] = derivs[corner, 1]
                    strain[2, column + 2] = derivs[corner, 2]
                    strain[3, column] = derivs[corner, 1]
                    strain[3, column + 1] = derivs[corner, 0]
                    strain[4, column + 1] = derivs[corner, 2]
                    strain[4, column + 2] = derivs[corner, 1]
                    strain[5, column] = derivs[corner, 2]
                    strain[5, column + 2] = derivs[corner, 0]
                stiffness = stiffness + strain.T @ elastic @ strain * 0.125
    return stiffness


def parity_operator():
    signs = np.ones((8, 8))
    for mode in range(8):
        for corner in range(8):
            for bit in range(3):
                if (mode >> bit) & 1:
                    signs[mode, corner] *= 2 * ((corner >> bit) & 1) - 1
    full = np.kron(signs, np.eye(3))
    coupled = full @ element_matrix() @ full.T / 64.0
    coupled[np.abs(coupled) < 1e-9] = 0.0
    return coupled


COUPLED = parity_operator()
LOW_END = tuple(math.tanh(sharpness * eta) for eta in thresholds)
DENOM = tuple(
    math.tanh(sharpness * eta) + math.tanh(sharpness * (1.0 - eta)) for eta in thresholds
)


def tent_rows(rows):
    for step in (1, 2, 1, 2):
        rows = [rows[i] + rows[i + step] for i in range(len(rows) - step)]
    return rows


def tent_sublanes(block, amount):
    size = block.shape[0]
    for step in (1, 2, 1, 2):
        block = block + pltpu.roll(block, size - step, 0)
    return block[:amount]


def lanes_up(parts, step, lane):
    rolled = [pltpu.roll(part, LANES - step, 1) for part in parts]
    rolled.append(jnp.zeros_like(parts[0]))
    return [
        jnp.where(lane < LANES - step, rolled[g], rolled[g + 1]) for g in range(len(parts))
    ]


def lanes_down(parts, step, lane):
    rolled = [jnp.zeros_like(parts[0])] + [pltpu.roll(part, step, 1) for part in parts]
    return [jnp.where(lane >= step, rolled[g + 1], rolled[g]) for g in range(len(parts))]


def tent_lanes(parts):
    lane = lax.broadcasted_iota(jnp.int32, parts[0].shape, 1)
    total = [4.0 * part for part in parts]
    for step in range(1, RAD + 1):
        ups, downs = lanes_up(parts, step, lane), lanes_down(parts, step, lane)
        if step == RAD:
            total = [t + (u + d) for t, u, d in zip(total, ups, downs)]
        else:
            total = [
                t + float(RAD + 1 - step) * (u + d) for t, u, d in zip(total, ups, downs)
            ]
    return total


def tent_weight(place, extent):
    total = jnp.zeros(place.shape, jnp.float32)
    for offset in range(-RAD, RAD + 1):
        inside = (place + offset >= 0) & (place + offset < extent)
        total = total + jnp.where(inside, float(RAD + 1 - abs(offset)), 0.0)
    return total


def halves(block):
    high = block.astype(jnp.bfloat16)
    low = (block - high.astype(jnp.float32)).astype(jnp.bfloat16)
    return jnp.concatenate([high, low], axis=1)


def lane_groups(depth):
    return [slice(g * LANES, (g + 1) * LANES) for g in range(depth // LANES)]


def modes_of(nodes, row, lane):
    fields = [[[None] * 3 for _ in range(2)] for _ in range(2)]
    for comp in range(3):
        value = nodes(comp, row)
        size = value.shape[0]
        ahead = jnp.where(lane < LANES - 1, pltpu.roll(value, LANES - 1, 1), 0.0)
        for mz, part in enumerate((value + ahead, ahead - value)):
            beside = pltpu.roll(part, size - 1, 0)
            fields[0][mz][comp] = part + beside
            fields[1][mz][comp] = beside - part
    return fields


def element_modes(low, high):
    modes = []
    for mx in range(2):
        for my in range(2):
            for mz in range(2):
                modes.append([
                    (h + l) if mx == 0 else (h - l)
                    for l, h in zip(low[my][mz], high[my][mz])
                ])
    return modes


def coupled_forces(modes):
    forces = [[None] * 3 for _ in range(8)]
    for mode in range(8):
        for comp in range(3):
            row = COUPLED[3 * mode + comp]
            groups = {}
            for place in np.nonzero(row)[0]:
                groups.setdefault(round(float(row[place]), 12), []).append(int(place))
            total = None
            for factor, places in groups.items():
                summed = modes[places[0] // 3][places[0] % 3]
                for place in places[1:]:
                    summed = summed + modes[place // 3][place % 3]
                term = factor * summed
                total = term if total is None else total + term
            forces[mode][comp] = total
    return forces


def pack_kernel(merged, n_narrow, design, passive, disp, support, up_ref, down_ref, *sides):
    rows, cols, depth = design.shape
    cx, cy, cz = support.shape
    groups = lane_groups(3 * cz)
    n = lax.axis_index("narrow")
    moved = lambda r, c, x: disp[r, c, x] * (1.0 - support[x].astype(jnp.float32))
    for k in range(RAD):
        up_ref[pl.ds(k * cols, cols), :] = design[rows - RAD + k]
        down_ref[pl.ds(k * cols, cols), :] = design[k]
    for r in range(3):
        for c in range(3):
            down_ref[pl.ds(RAD * cols + r * cy, cy), groups[c]] = moved(r, c, 0)

    def edge(high, low, kind):
        if kind == "merged":
            return jnp.where(n == 0, high, low)
        return high if kind == "high" else low

    kinds = ("merged",) if merged else ("high", "low")
    for index, kind in enumerate(kinds):
        side, side_up, side_down = sides[3 * index : 3 * index + 3]
        for k in range(rows):
            piece = edge(design[k, cols - REACH :, :], design[k, :REACH, :], kind)
            side[pl.ds(k * REACH, REACH), :] = piece
            if k < RAD:
                side_down[pl.ds(k * REACH, REACH), :] = piece
            if k >= rows - RAD:
                side_up[pl.ds((k - rows + RAD) * REACH, REACH), :] = piece
            mask = edge(passive[k, cols - RAD :, :], passive[k, :RAD, :], kind)
            side[pl.ds(rows * REACH + k * RAD, RAD), :] = 1.0 - mask.astype(jnp.float32)
        base = rows * (REACH + RAD)
        for r in range(3):
            for c in range(3):
                for x in range(cx):
                    value = moved(r, c, x)
                    piece = edge(value[cy - 2 :], value[:2], kind)
                    side[pl.ds(base + (r * cx + x) * 2, 2), groups[c]] = piece
                    if x == 0:
                        side_down[pl.ds(RAD * REACH + 2 * r, 2), groups[c]] = piece
        used = base + 6 * cx
        if side.shape[0] > used:
            side[used:, :] = jnp.zeros((side.shape[0] - used, depth), jnp.float32)
        used = RAD * REACH
        if side_up.shape[0] > used:
            side_up[used:, :] = jnp.zeros((side_up.shape[0] - used, depth), jnp.float32)
        used = RAD * REACH + 6
        if side_down.shape[0] > used:
            side_down[used:, :] = jnp.zeros((side_down.shape[0] - used, depth), jnp.float32)


def project_kernel(
    n_wide, n_narrow, design, passive, disp, support, from_low, from_high,
    side_b, side_a, up_b, up_a, down_b, down_a,
    gg_ref, nodes_ref, energy_ref, moduli_ref, part_ref,
    blurred, mask_ref, cubes, packed, agg,
):
    rows, cols, depth = design.shape
    cx, cy, cz = support.shape
    groups = lane_groups(depth)
    n = lax.axis_index("narrow")
    w = lax.axis_index("wide")
    valid_b = jnp.where(n > 0, 1.0, 0.0)
    valid_a = jnp.where(n < n_narrow - 1, 1.0, 0.0)
    ext = mask_ref.shape[1]

    nodes_ref[...] = jnp.zeros_like(nodes_ref)
    base = rows * (REACH + RAD)
    for r in range(3):
        for c in range(3):
            lanes = groups[c]
            for x in range(cx):
                free = 1.0 - support[x].astype(jnp.float32)
                nodes_ref[r, c, x, 1 : cy + 1, :] = disp[r, c, x] * free
                at = base + (r * cx + x) * 2
                nodes_ref[r, c, x, 0:1, :] = side_b[at + 1 : at + 2, lanes] * valid_b
                nodes_ref[r, c, x, cy + 1 : cy + 3, :] = side_a[at : at + 2, lanes] * valid_a
            at = RAD * cols + r * cy
            nodes_ref[r, c, cx, 1 : cy + 1, :] = from_high[at : at + cy, lanes]
            at = RAD * REACH + 2 * r
            nodes_ref[r, c, cx, 0:1, :] = down_b[at + 1 : at + 2, lanes] * valid_b
            nodes_ref[r, c, cx, cy + 1 : cy + 3, :] = down_a[at : at + 2, lanes] * valid_a

    lane = lax.broadcasted_iota(jnp.int32, nodes_ref.shape[3:], 1)
    for r in range(3):
        low = modes_of(lambda c, x: nodes_ref[r, c, x], 0, lane)
        for x in range(cx):
            high = modes_of(lambda c, x: nodes_ref[r, c, x], x + 1, lane)
            modes = element_modes(low, high)
            forces = coupled_forces(modes)
            total = None
            for mode in range(8):
                for comp in range(3):
                    if forces[mode][comp] is not None:
                        term = modes[mode][comp] * forces[mode][comp]
                        total = term if total is None else total + term
            energy_ref[r * cx + x] = total
            low = high

    for start in range(0, cols, 8):
        for lanes in groups:
            column = [from_low[k * cols + start : k * cols + start + 8, lanes] for k in range(RAD)]
            column += [design[k, start : start + 8, lanes] for k in range(rows)]
            column += [from_high[k * cols + start : k * cols + start + 8, lanes] for k in range(RAD)]
            for k, value in enumerate(tent_rows(column)):
                blurred[k, REACH + start : REACH + start + 8, lanes] = value
    for at, side, up, down, valid in (
        (0, side_b, up_b, down_b, valid_b),
        (REACH + cols, side_a, up_a, down_a, valid_a),
    ):
        for lanes in groups:
            pick = lambda ref, k: ref[k * REACH : (k + 1) * REACH, lanes] * valid
            column = [pick(up, k) for k in range(RAD)]
            column += [pick(side, k) for k in range(rows)]
            column += [pick(down, k) for k in range(RAD)]
            for k, value in enumerate(tent_rows(column)):
                blurred[k, at : at + REACH, lanes] = value
    tail = blurred.shape[1] - cols - 2 * REACH
    if tail:
        blurred[:, cols + 2 * REACH :, :] = jnp.zeros((rows, tail, depth), jnp.float32)

    for k in range(rows):
        mask_ref[k, RAD : RAD + cols, :] = 1.0 - passive[k].astype(jnp.float32)
        at = rows * REACH + k * RAD
        mask_ref[k, 0:RAD, :] = side_b[at : at + RAD, :]
        mask_ref[k, RAD + cols : 2 * RAD + cols, :] = side_a[at : at + RAD, :]
        mask_ref[k, 2 * RAD + cols :, :] = jnp.zeros((ext - 2 * RAD - cols, depth), jnp.float32)

    place_y = n * cols - RAD + lax.broadcasted_iota(jnp.int32, (ext, LANES), 0)
    extent_y = n_narrow * cols
    inside = (place_y >= 0) & (place_y < extent_y)
    weight_y = tent_weight(place_y, extent_y)
    recip_y = jnp.where(inside, 1.0 / jnp.maximum(weight_y, 1.0), 0.0)
    recip_z = []
    for g in range(len(groups)):
        place_z = g * LANES + lax.broadcasted_iota(jnp.int32, (ext, LANES), 1)
        recip_z.append(1.0 / tent_weight(place_z, depth))

    def coarse_row(x, carry):
        for sub in range(3):
            k = 3 * x + sub
            parts = [tent_sublanes(blurred[k, :, lanes], ext) for lanes in groups]
            parts = tent_lanes(parts)
            place_x = w * rows + k + jnp.zeros((8, LANES), jnp.int32)
            recip_x = (1.0 / tent_weight(place_x, n_wide * rows))[0:1]
            recip_xy = recip_y * recip_x
            for g, lanes in enumerate(groups):
                recip = recip_xy * recip_z[g]
                scaled = (sharpness * recip) * parts[g]
                mask = mask_ref[k, :, lanes]
                for r in range(3):
                    steep = jnp.tanh(scaled - sharpness * thresholds[r])
                    dense = (steep + LOW_END[r]) * mask
                    square = dense * dense
                    cube = square * dense
                    gg_ref[r, k, :, lanes] = square * (1.0 - steep * steep) * recip
                    at = r * cx + x
                    if sub == 0:
                        cubes[at, g] = cube
                    else:
                        cubes[at, g] = cubes[at, g] + cube
        return carry

    lax.fori_loop(0, cx, coarse_row, 0)

    padded = moduli_ref.shape[1]
    reach = cy + 2
    row_id = lax.broadcasted_iota(jnp.int32, (LANES, LANES), 0)
    col_id = lax.broadcasted_iota(jnp.int32, (LANES, LANES), 1)
    total = None
    packed[...] = jnp.zeros_like(packed)
    for g in range(len(groups)):
        for at in range(3 * cx):
            summed = cubes[at, g, pl.ds(0, reach, stride=3), :]
            summed = summed + cubes[at, g, pl.ds(1, reach, stride=3), :]
            summed = summed + cubes[at, g, pl.ds(2, reach, stride=3), :]
            packed[at * padded : at * padded + reach, :] = summed
        gather = ((g * LANES + row_id) // 3 == col_id).astype(jnp.float32).astype(jnp.bfloat16)
        term = jnp.dot(
            halves(packed[...]),
            jnp.concatenate([gather, gather], axis=0),
            preferred_element_type=jnp.float32,
        )
        total = term if total is None else total + term
    agg[...] = total
    sub_id = lax.broadcasted_iota(jnp.int32, (padded, LANES), 0)
    outside = jnp.where(n > 0, -1, 0)
    own = ((sub_id >= 1) & (sub_id <= cy)).astype(jnp.float32)
    part_ref[...] = jnp.zeros_like(part_ref)
    for r in range(3):
        partial = None
        for x in range(cx):
            at = r * cx + x
            value = agg[at * padded : (at + 1) * padded, :]
            value = stiff_floor + ((1.0 - stiff_floor) / 27.0 / DENOM[r] ** 3) * value
            value = jnp.where((sub_id > outside) & (sub_id < reach), value, 0.0)
            moduli_ref[at] = value
            term = value * energy_ref[at]
            partial = term if partial is None else partial + term
        part_ref[r : r + 1, :] = jnp.sum(partial * own, axis=0, keepdims=True)


def force_kernel(
    gg, nodes_ref, energy, moduli, support, loading,
    h_ref, up_ref, down_ref, residual_ref, spread_ref, packed,
):
    _, rows, ext, depth = gg.shape
    cx, cy, cz = support.shape
    padded = moduli.shape[1]
    reach = cy + 2
    groups = lane_groups(depth)

    row_id = lax.broadcasted_iota(jnp.int32, (LANES, LANES), 0)
    col_id = lax.broadcasted_iota(jnp.int32, (LANES, LANES), 1)
    for at in range(3 * cx):
        packed[at * padded : (at + 1) * padded, :] = energy[at]
    split = halves(packed[...])
    for g in range(len(groups)):
        copies = (row_id == (g * LANES + col_id) // 3).astype(jnp.float32).astype(jnp.bfloat16)
        fine = jnp.dot(
            split, jnp.concatenate([copies, copies], axis=0), preferred_element_type=jnp.float32
        )
        for at in range(3 * cx):
            value = fine[at * padded : at * padded + reach]
            for sub in range(3):
                spread_ref[at, g, pl.ds(sub, reach, stride=3), :] = value
            if 3 * reach < ext:
                spread_ref[at, g, 3 * reach :, :] = jnp.zeros((ext - 3 * reach, LANES), jnp.float32)

    for r in range(3):
        def fine_rows(x, carry):
            for sub in range(3):
                for g, lanes in enumerate(groups):
                    k = 3 * x + sub
                    h_ref[r, k, :, lanes] = gg[r, k, :, lanes] * spread_ref[r * cx + x, g]
            return carry

        lax.fori_loop(0, cx, fine_rows, 0)
        for k in range(RAD):
            at = (r * RAD + k) * ext
            up_ref[at : at + ext, :] = h_ref[r, rows - RAD + k]
            down_ref[at : at + ext, :] = h_ref[r, k]

    lane = lax.broadcasted_iota(jnp.int32, nodes_ref.shape[3:], 1)
    for r in range(3):
        nodes = lambda c, x: nodes_ref[r, c, x]
        low = modes_of(nodes, 0, lane)
        above = None
        for x in range(cx + 1):
            sums = [[[None] * 3 for _ in range(2)] for _ in range(2)]
            below, above_next = above, None
            if x < cx:
                high = modes_of(nodes, x + 1, lane)
                forces = coupled_forces(element_modes(low, high))
                low = high
                modulus = moduli[r * cx + x]
                scaled = [
                    [None if f is None else modulus * f for f in mode] for mode in forces
                ]
                above_next = [[[None] * 3 for _ in range(2)] for _ in range(2)]
                for my in range(2):
                    for mz in range(2):
                        for comp in range(3):
                            even = scaled[2 * my + mz][comp]
                            odd = scaled[4 + 2 * my + mz][comp]
                            if even is None:
                                sums[my][mz][comp] = -odd
                                above_next[my][mz][comp] = odd
                            else:
                                sums[my][mz][comp] = even - odd
                                above_next[my][mz][comp] = even + odd
            for comp in range(3):
                along = [None, None]
                for mz in range(2):
                    pair = []
                    for my in range(2):
                        value = sums[my][mz][comp]
                        if below is not None:
                            other = below[my][mz][comp]
                            value = other if value is None else value + other
                        pair.append(value)
                    along[mz] = (pair[0] - pair[1]) + pltpu.roll(pair[0] + pair[1], 1, 0)
                total = (along[0] - along[1]) + jnp.where(
                    lane >= 1, pltpu.roll(along[0] + along[1], 1, 1), 0.0
                )
                total = total[1 : cy + 1]
                if x < cx:
                    free = 1.0 - support[x].astype(jnp.float32)
                    if comp == 2:
                        total = total + load_force * loading[x].astype(jnp.float32)
                    residual_ref[r, comp, x] = -total * free
                else:
                    at = 3 * RAD * ext + r * cy
                    up_ref[at : at + cy, groups[comp]] = total
            above = above_next


def blur_kernel(
    h_ref, low_ref, high_ref, residual_in, support, fields_ref, residual_ref, summed
):
    _, rows, ext, depth = h_ref.shape
    cx, cy, cz = support.shape
    cols = fields_ref.shape[2]
    groups = lane_groups(depth)
    residual_ref[...] = residual_in[...]
    free = 1.0 - support[0].astype(jnp.float32)
    for r in range(3):
        at = 3 * RAD * ext + r * cy
        for comp in range(3):
            residual_ref[r, comp, 0] = (
                residual_in[r, comp, 0] - low_ref[at : at + cy, groups[comp]] * free
            )
    for r in range(3):
        def first_dim(s, carry):
            start = pl.multiple_of(8 * s, 8)
            for lanes in groups:
                column = [
                    low_ref[pl.ds((r * RAD + k) * ext + start, 8), lanes] for k in range(RAD)
                ]
                column += [h_ref[r, k, pl.ds(start, 8), lanes] for k in range(rows)]
                column += [
                    high_ref[pl.ds((r * RAD + k) * ext + start, 8), lanes] for k in range(RAD)
                ]
                for k, value in enumerate(tent_rows(column)):
                    summed[k, pl.ds(start, 8), lanes] = value
            return carry

        lax.fori_loop(0, ext // 8, first_dim, 0)

        def other_dims(k, carry):
            parts = [tent_sublanes(summed[k, :, lanes], cols) for lanes in groups]
            for lanes, part in zip(groups, tent_lanes(parts)):
                fields_ref[r, k, :, lanes] = part
            return carry

        lax.fori_loop(0, rows, other_dims, 0)


def call(kernel, shapes, scratch, flops, args, name):
    vmem = pl.BlockSpec(memory_space=pltpu.VMEM)
    return pl.pallas_call(
        kernel,
        out_shape=[jax.ShapeDtypeStruct(s, jnp.float32) for s in shapes],
        in_specs=[vmem] * len(args),
        out_specs=[vmem] * len(shapes),
        scratch_shapes=[pltpu.VMEM(s, jnp.float32) for s in scratch],
        compiler_params=pltpu.CompilerParams(vmem_limit_bytes=48 * 1024 * 1024),
        cost_estimate=pl.CostEstimate(flops=flops, bytes_accessed=1000000, transcendentals=0),
        name=name,
    )(*args)


def ceil8(amount):
    return -(-amount // 8) * 8


def all_sum(value, n_wide, n_narrow):
    total = n_wide * n_narrow
    axes = ("wide", "narrow")
    if total & (total - 1):
        return lax.psum(value, axes)
    step = 1
    while step < total:
        value = value + lax.ppermute(value, axes, [(i, i ^ step) for i in range(total)])
        step *= 2
    return value


def local(n_wide, n_narrow, design, passive, displacement, support, loading):
    rows, cols, depth = design.shape
    cx, cy, cz = support.shape
    merged = n_narrow == 2
    axes = ("wide", "narrow")
    ext = ceil8(cols + 2 * RAD)
    padded = ceil8(cy + 3)

    def route(dx, dy):
        pairs = []
        for i in range(n_wide):
            for j in range(n_narrow):
                if 0 <= i + dx < n_wide and 0 <= j + dy < n_narrow:
                    pairs.append((i * n_narrow + j, (i + dx) * n_narrow + j + dy))
        return pairs

    def side_route(dx, index):
        if merged:
            return route(dx, 1) + route(dx, -1)
        return route(dx, 1 if index == 0 else -1)

    sides = 1 if merged else 2
    side_shapes = [
        (ceil8(rows * (REACH + RAD) + 6 * cx), depth),
        (ceil8(RAD * REACH), depth),
        (ceil8(RAD * REACH + 6), depth),
    ]
    packs = call(
        functools.partial(pack_kernel, merged, n_narrow),
        [(RAD * cols, depth), (RAD * cols + 3 * cy, depth)] + side_shapes * sides,
        [], 200000, (design, passive, displacement, support), "pack",
    )
    send = lambda block, pairs: lax.ppermute(block, axes, pairs)
    from_low = send(packs[0], route(1, 0))
    from_high = send(packs[1], route(-1, 0))
    got = []
    for index in range(sides):
        side, side_up, side_down = packs[2 + 3 * index : 5 + 3 * index]
        got.append((
            send(side, side_route(0, index)),
            send(side_up, side_route(1, index)),
            send(side_down, side_route(-1, index)),
        ))
    before, after = got[0], got[-1]
    gg, nodes, energy, moduli, part = call(
        functools.partial(project_kernel, n_wide, n_narrow),
        [
            (3, rows, ext, depth), (3, 3, cx + 1, padded, cz), (3 * cx, padded, cz),
            (3 * cx, padded, cz), (8, LANES),
        ],
        [
            (rows, ceil8(cols + 2 * REACH), depth), (rows, ext, depth),
            (3 * cx, depth // LANES, ext, LANES), (3 * cx * padded, LANES),
            (3 * cx * padded, LANES),
        ],
        20000000,
        (
            design, passive, displacement, support, from_low, from_high,
            before[0], after[0], before[1], after[1], before[2], after[2],
        ),
        "project",
    )
    summed = all_sum(part, n_wide, n_narrow)
    h, up, down, residual = call(
        force_kernel,
        [
            (3, rows, ext, depth), (3 * RAD * ext + 3 * cy, depth), (3 * RAD * ext, depth),
            displacement.shape,
        ],
        [(3 * cx, depth // LANES, ext, LANES), (3 * cx * padded, LANES)],
        10000000, (gg, nodes, energy, moduli, support, loading), "force",
    )
    low = send(up, route(1, 0))
    high = send(down, route(-1, 0))
    fields, residual = call(
        blur_kernel,
        [(3, rows, cols, depth), displacement.shape],
        [(rows, ext, depth)],
        10000000, (h, low, high, residual, support), "blur",
    )
    compliance = jnp.sum(summed[:3], axis=1)
    sensitivity = None
    for r in range(3):
        factor = 3.0 * (1.0 - stiff_floor) / 27.0 * sharpness / DENOM[r] ** 3
        term = (-factor / compliance[r]) * fields[r]
        sensitivity = term if sensitivity is None else sensitivity + term
    return residual, compliance, sensitivity


def solution(mesh):
    in_specs = (
        P("wide", "narrow", None),
        P("wide", "narrow", None),
        P(None, None, "wide", "narrow", None),
        P("wide", "narrow", None),
        P("wide", "narrow", None),
    )
    out_specs = (P(None, None, "wide", "narrow", None), P(), P("wide", "narrow", None))
    body = functools.partial(local, mesh.shape["wide"], mesh.shape["narrow"])
    return jax.shard_map(body, mesh=mesh, in_specs=in_specs, out_specs=out_specs, check_vma=False)
```

```python
import functools
import math

import jax
import jax.numpy as jnp
import numpy as np
from jax import lax
from jax.experimental import pallas as pl
from jax.experimental.pallas import tpu as pltpu
from jax.sharding import PartitionSpec as P


RAD = 3
sharpness = 8.0
thresholds = (0.7, 0.5, 0.3)
stiff_floor = 0.001
load_force = 4.0
poisson = 0.3
LANES = 128
REACH = 2 * RAD


def element_matrix():
    inv_root = 1.0 / np.sqrt(3.0)
    elastic_scale = 1.0 / ((1.0 + poisson) * (1.0 - 2.0 * poisson))
    elastic = np.zeros((6, 6))
    for row_i in range(3):
        for col_j in range(3):
            elastic[row_i, col_j] = poisson
        elastic[row_i, row_i] = 1.0 - poisson
    for row_i in range(3, 6):
        elastic[row_i, row_i] = 0.5 - poisson
    elastic = elastic * elastic_scale
    corner_signs = [
        (2 * (corner // 4) - 1, 2 * (corner // 2 % 2) - 1, 2 * (corner % 2) - 1)
        for corner in range(8)
    ]
    stiffness = np.zeros((24, 24))
    for gauss_a in (-inv_root, inv_root):
        for gauss_b in (-inv_root, inv_root):
            for gauss_c in (-inv_root, inv_root):
                gauss_point = (gauss_a, gauss_b, gauss_c)
                derivs = np.zeros((8, 3))
                for corner in range(8):
                    for along in range(3):
                        slope_value = corner_signs[corner][along] / 8.0
                        for second in range(3):
                            if second != along:
                                slope_value = slope_value * (
                                    1.0 + corner_signs[corner][second] * gauss_point[second]
                                )
                        derivs[corner, along] = 2.0 * slope_value
                strain = np.zeros((6, 24))
                for corner in range(8):
                    column = 3 * corner
                    strain[0, column] = derivs[corner, 0]
                    strain[1, column + 1] = derivs[corner, 1]
                    strain[2, column + 2] = derivs[corner, 2]
                    strain[3, column] = derivs[corner, 1]
                    strain[3, column + 1] = derivs[corner, 0]
                    strain[4, column + 1] = derivs[corner, 2]
                    strain[4, column + 2] = derivs[corner, 1]
                    strain[5, column] = derivs[corner, 2]
                    strain[5, column + 2] = derivs[corner, 0]
                stiffness = stiffness + strain.T @ elastic @ strain * 0.125
    return stiffness


def parity_operator():
    signs = np.ones((8, 8))
    for mode in range(8):
        for corner in range(8):
            for bit in range(3):
                if (mode >> bit) & 1:
                    signs[mode, corner] *= 2 * ((corner >> bit) & 1) - 1
    full = np.kron(signs, np.eye(3))
    coupled = full @ element_matrix() @ full.T / 64.0
    coupled[np.abs(coupled) < 1e-9] = 0.0
    return coupled


COUPLED = parity_operator()
LOW_END = tuple(math.tanh(sharpness * eta) for eta in thresholds)
DENOM = tuple(
    math.tanh(sharpness * eta) + math.tanh(sharpness * (1.0 - eta)) for eta in thresholds
)


def tent_rows(rows):
    for step in (1, 2, 1, 2):
        rows = [rows[i] + rows[i + step] for i in range(len(rows) - step)]
    return rows


def tent_sublanes(block, amount):
    size = block.shape[0]
    for step in (1, 2, 1, 2):
        block = block + pltpu.roll(block, size - step, 0)
    return block[:amount]


def lanes_up(parts, step, lane):
    rolled = [pltpu.roll(part, LANES - step, 1) for part in parts]
    rolled.append(jnp.zeros_like(parts[0]))
    return [
        jnp.where(lane < LANES - step, rolled[g], rolled[g + 1]) for g in range(len(parts))
    ]


def lanes_down(parts, step, lane):
    rolled = [jnp.zeros_like(parts[0])] + [pltpu.roll(part, step, 1) for part in parts]
    return [jnp.where(lane >= step, rolled[g + 1], rolled[g]) for g in range(len(parts))]


def tent_lanes(parts):
    lane = lax.broadcasted_iota(jnp.int32, parts[0].shape, 1)
    total = [4.0 * part for part in parts]
    for step in range(1, RAD + 1):
        ups, downs = lanes_up(parts, step, lane), lanes_down(parts, step, lane)
        if step == RAD:
            total = [t + (u + d) for t, u, d in zip(total, ups, downs)]
        else:
            total = [
                t + float(RAD + 1 - step) * (u + d) for t, u, d in zip(total, ups, downs)
            ]
    return total


def tent_weight(place, extent):
    total = jnp.zeros(place.shape, jnp.float32)
    for offset in range(-RAD, RAD + 1):
        inside = (place + offset >= 0) & (place + offset < extent)
        total = total + jnp.where(inside, float(RAD + 1 - abs(offset)), 0.0)
    return total


def halves(block):
    high = block.astype(jnp.bfloat16)
    low = (block - high.astype(jnp.float32)).astype(jnp.bfloat16)
    return jnp.concatenate([high, low], axis=1)


def lane_groups(depth):
    return [slice(g * LANES, (g + 1) * LANES) for g in range(depth // LANES)]


def modes_of(nodes, row, lane):
    fields = [[[None] * 3 for _ in range(2)] for _ in range(2)]
    for comp in range(3):
        value = nodes(comp, row)
        size = value.shape[0]
        ahead = jnp.where(lane < LANES - 1, pltpu.roll(value, LANES - 1, 1), 0.0)
        for mz, part in enumerate((value + ahead, ahead - value)):
            beside = pltpu.roll(part, size - 1, 0)
            fields[0][mz][comp] = part + beside
            fields[1][mz][comp] = beside - part
    return fields


def element_modes(low, high):
    modes = []
    for mx in range(2):
        for my in range(2):
            for mz in range(2):
                modes.append([
                    (h + l) if mx == 0 else (h - l)
                    for l, h in zip(low[my][mz], high[my][mz])
                ])
    return modes


def coupled_forces(modes):
    forces = [[None] * 3 for _ in range(8)]
    for mode in range(8):
        for comp in range(3):
            row = COUPLED[3 * mode + comp]
            groups = {}
            for place in np.nonzero(row)[0]:
                groups.setdefault(round(float(row[place]), 12), []).append(int(place))
            total = None
            for factor, places in groups.items():
                summed = modes[places[0] // 3][places[0] % 3]
                for place in places[1:]:
                    summed = summed + modes[place // 3][place % 3]
                term = factor * summed
                total = term if total is None else total + term
            forces[mode][comp] = total
    return forces


def pick(n, high, low, kind):
    if kind == "merged":
        return jnp.where(n == 0, high, low)
    return high if kind == "high" else low


def column_start(n, cols, kind):
    if kind == "merged":
        return pl.multiple_of(jnp.where(n == 0, cols - 8, 0), 8)
    return cols - 8 if kind == "high" else 0


def fill_tail(ref, used):
    if ref.shape[0] > used:
        ref[used:, :] = jnp.zeros((ref.shape[0] - used, ref.shape[1]), jnp.float32)


def pack_kernel(
    kinds, design, passive, disp, support, near_ref, far_ref, row_ref, nodes_ref, *rest
):
    rows, cols, depth = design.shape
    cx, cy, _ = support.shape
    sides, (edges, masks, moves, frees, sems) = rest[: 3 * len(kinds)], rest[3 * len(kinds) :]
    groups = lane_groups(depth)
    n = lax.axis_index("narrow")
    even = lax.rem(lax.axis_index("wide"), 2) == 0
    near_start = jnp.where(even, rows - RAD, 0)
    far_start = jnp.where(even, 0, rows - RAD)
    copies = [
        pltpu.make_async_copy(disp, moves, sems.at[0]),
        pltpu.make_async_copy(support, frees, sems.at[1]),
    ]
    for index, kind in enumerate(kinds):
        start = column_start(n, cols, kind)
        copies.append(
            pltpu.make_async_copy(
                design.at[:, pl.ds(start, 8), :], edges.at[index], sems.at[2 + 2 * index]
            )
        )
        copies.append(
            pltpu.make_async_copy(
                passive.at[:, pl.ds(start, 8), :], masks.at[index], sems.at[3 + 2 * index]
            )
        )
    last = 2 + 2 * len(kinds)
    for at, start, ref in ((last, near_start, near_ref), (last + 1, far_start, far_ref)):
        copies.append(
            pltpu.make_async_copy(design.at[pl.ds(start, RAD)], ref.at[:RAD], sems.at[at])
        )
    for copy in copies:
        copy.start()
    nodes_ref[...] = jnp.zeros_like(nodes_ref)
    for copy in copies[:2]:
        copy.wait()
    for x in range(cx):
        free = 1.0 - frees[x].astype(jnp.float32)
        for r in range(3):
            for c in range(3):
                value = moves[r, c, x] * free
                nodes_ref[r, c, x, 1 : cy + 1, :] = value
                if x == 0:
                    near_ref[RAD, r * cy : (r + 1) * cy, groups[c]] = value
                    row_ref[r * cy : (r + 1) * cy, groups[c]] = value
    for copy in copies[2:last]:
        copy.wait()

    for index, kind in enumerate(kinds):
        side, side_near, side_far = sides[3 * index : 3 * index + 3]
        for k in range(rows):
            value = edges[index, k]
            piece = pick(n, value[8 - REACH :], value[:REACH], kind)
            side[pl.ds(k * REACH, REACH), :] = piece
            value = 1.0 - masks[index, k].astype(jnp.float32)
            side[pl.ds(rows * REACH + k * RAD, RAD), :] = pick(n, value[8 - RAD :], value[:RAD], kind)
        for k in range(RAD):
            for ref, start in ((side_near, near_start), (side_far, far_start)):
                value = edges[index, start + k]
                piece = pick(n, value[8 - REACH :], value[:REACH], kind)
                ref[pl.ds(k * REACH, REACH), :] = piece
        base = rows * (REACH + RAD)
        for r in range(3):
            for c in range(3):
                for x in range(cx):
                    value = nodes_ref[r, c, x]
                    piece = pick(n, value[cy - 1 : cy + 1], value[1:3], kind)
                    side[pl.ds(base + (r * cx + x) * 2, 2), groups[c]] = piece
                    if x == 0:
                        side_near[pl.ds(RAD * REACH + 2 * r, 2), groups[c]] = piece
                        side_far[pl.ds(RAD * REACH + 2 * r, 2), groups[c]] = piece
        fill_tail(side, base + 6 * cx)
        fill_tail(side_near, RAD * REACH + 6)
        fill_tail(side_far, RAD * REACH + 6)
    for copy in copies[last:]:
        copy.wait()


def element_energy(low, high):
    modes = element_modes(low, high)
    forces = coupled_forces(modes)
    total = None
    for mode in range(8):
        for comp in range(3):
            if forces[mode][comp] is not None:
                term = modes[mode][comp] * forces[mode][comp]
                total = term if total is None else total + term
    return total


def reciprocal_weight(place, extent):
    inside = (place >= 0) & (place < extent)
    return jnp.where(inside, 1.0 / jnp.maximum(tent_weight(place, extent), 1.0), 0.0)


def plane_reciprocals(n, n_narrow, cols, ext, depth):
    place_y = n * cols - RAD + lax.broadcasted_iota(jnp.int32, (ext, LANES), 0)
    recip_y = reciprocal_weight(place_y, n_narrow * cols)
    recip_z = []
    for g in range(depth // LANES):
        place_z = g * LANES + lax.broadcasted_iota(jnp.int32, (ext, LANES), 1)
        recip_z.append(1.0 / tent_weight(place_z, depth))
    return recip_y, recip_z


def low_ends():
    return [jnp.tanh(jnp.full((1, LANES), sharpness * eta, jnp.float32)) for eta in thresholds]


def project_row(row, recip_x, recips, lows, emit, groups):
    recip_y, recip_z = recips
    recip_xy = recip_y * recip_x
    for g, lanes in enumerate(groups):
        recip = recip_xy * recip_z[g]
        scaled = sharpness * row(lanes)
        for r in range(3):
            steep = jnp.tanh(scaled - sharpness * thresholds[r])
            dense = steep + lows[r]
            square = dense * dense
            emit(r, g, lanes, square * (1.0 - steep * steep) * recip, square * dense)


def element_sums(cubes, amount, packed, reach, padded):
    row_id = lax.broadcasted_iota(jnp.int32, (LANES, LANES), 0)
    col_id = lax.broadcasted_iota(jnp.int32, (LANES, LANES), 1)
    total = None
    packed[...] = jnp.zeros_like(packed)
    for g in range(cubes.shape[1]):
        for at in range(amount):
            summed = cubes[at, g, pl.ds(0, reach, stride=3), :]
            summed = summed + cubes[at, g, pl.ds(1, reach, stride=3), :]
            summed = summed + cubes[at, g, pl.ds(2, reach, stride=3), :]
            packed[at * padded : at * padded + reach, :] = summed
        gather = ((g * LANES + row_id) // 3 == col_id).astype(jnp.float32).astype(jnp.bfloat16)
        term = jnp.dot(
            halves(packed[...]),
            jnp.concatenate([gather, gather], axis=0),
            preferred_element_type=jnp.float32,
        )
        total = term if total is None else total + term
    return total


def modulus_of(value, r, keep):
    value = stiff_floor + ((1.0 - stiff_floor) / 27.0 / DENOM[r] ** 3) * value
    return jnp.where(keep, value, 0.0)


def load_kernel(design_hbm, passive_hbm, design, mask_ref, passive, sems):
    rows, cols, depth = design.shape
    copies = [
        pltpu.make_async_copy(passive_hbm, passive, sems.at[0]),
        pltpu.make_async_copy(design_hbm, design, sems.at[1]),
    ]
    for copy in copies:
        copy.start()
    copies[0].wait()
    for k in range(rows):
        mask_ref[k, RAD : RAD + cols, :] = 1.0 - passive[k].astype(jnp.float32)
        mask_ref[k, :RAD, :] = jnp.zeros((RAD, depth), jnp.float32)
        tail = mask_ref.shape[1] - RAD - cols
        mask_ref[k, RAD + cols :, :] = jnp.zeros((tail, depth), jnp.float32)
    copies[1].wait()


def blur_kernel(
    n_wide, n_narrow, design, mask_in, nodes_in, near, far,
    side_b, side_a, near_b, near_a, far_b, far_a,
    v_ref, nodes_ref, near_ref, far_ref, ends, corners, blurred, edge_mask,
):
    rows, cols, depth = design.shape
    cx = nodes_ref.shape[2]
    cy = cols // 3
    groups = lane_groups(depth)
    n = lax.axis_index("narrow")
    w = lax.axis_index("wide")
    valid_b = jnp.where(n > 0, 1.0, 0.0)
    valid_a = jnp.where(n < n_narrow - 1, 1.0, 0.0)
    ext = v_ref.shape[1]

    above = 1 - lax.rem(w, 2)
    for index, ref in ((above, near), (1 - above, far)):
        for k in range(RAD):
            ends[index, k] = ref[k]
    for index, pair in ((above, (near_b, near_a)), (1 - above, (far_b, far_a))):
        for which, ref in enumerate(pair):
            corners[which, index] = ref[...] * (valid_b, valid_a)[which]

    base = rows * (REACH + RAD)
    for r in range(3):
        for c in range(3):
            lanes = groups[c]
            for x in range(cx):
                nodes_ref[r, c, x] = nodes_in[r, c, x]
                at = base + (r * cx + x) * 2
                nodes_ref[r, c, x, 0:1, :] = side_b[at + 1 : at + 2, lanes] * valid_b
                nodes_ref[r, c, x, cy + 1 : cy + 3, :] = side_a[at : at + 2, lanes] * valid_a

    for start in range(0, cols, 8):
        place = slice(start, start + 8)
        for lanes in groups:
            column = [ends[0, k, place, lanes] for k in range(RAD)]
            column += [design[k, place, lanes] for k in range(rows)]
            column += [ends[1, k, place, lanes] for k in range(RAD)]
            for k, value in enumerate(tent_rows(column)):
                blurred[k, REACH + start : REACH + start + 8, lanes] = value
    span = lambda k: slice(k * REACH, (k + 1) * REACH)
    for which, at, side, valid in ((0, 0, side_b, valid_b), (1, REACH + cols, side_a, valid_a)):
        for lanes in groups:
            column = [corners[which, 0, span(k), lanes] for k in range(RAD)]
            column += [side[span(k), lanes] * valid for k in range(rows)]
            column += [corners[which, 1, span(k), lanes] for k in range(RAD)]
            for k, value in enumerate(tent_rows(column)):
                blurred[k, at : at + REACH, lanes] = value
    tail = blurred.shape[1] - cols - 2 * REACH
    if tail:
        blurred[:, cols + 2 * REACH :, :] = jnp.zeros((rows, tail, depth), jnp.float32)

    edge_mask[...] = mask_in[...]
    for k in range(rows):
        at = rows * REACH + k * RAD
        edge_mask[k, 0:RAD, :] = side_b[at : at + RAD, :]
        edge_mask[k, RAD + cols : 2 * RAD + cols, :] = side_a[at : at + RAD, :]

    recip_y, recip_z = plane_reciprocals(n, n_narrow, cols, ext, depth)

    def fine_row(x, carry):
        for sub in range(3):
            k = 3 * x + sub
            parts = tent_lanes([tent_sublanes(blurred[k, :, lanes], ext) for lanes in groups])
            place_x = w * rows + k + jnp.zeros((8, LANES), jnp.int32)
            recip_x = reciprocal_weight(place_x, n_wide * rows)[0:1]
            recip_xy = recip_y * recip_x
            for g, lanes in enumerate(groups):
                v_ref[k, :, lanes] = (recip_xy * recip_z[g]) * parts[g] * edge_mask[k, :, lanes]
        return carry

    for x in range(cx):
        fine_row(x, 0)

    near_first, near_x = above * (rows - RAD), 1 + above * (cx - 2)
    for ref, first, x in (
        (near_ref, near_first, near_x), (far_ref, rows - RAD - near_first, cx - near_x)
    ):
        for k in range(RAD):
            ref[k * ext : (k + 1) * ext, :] = v_ref[first + k]
        for r in range(3):
            at = RAD * ext + r * nodes_ref.shape[3]
            for c in range(3):
                ref[at : at + nodes_ref.shape[3], groups[c]] = nodes_ref[r, c, x]


def project_kernel(
    n_wide, n_narrow, v_ref, nodes_in, near, row, near_b, near_a, far_b, far_a,
    gg_ref, moduli_ref, part_ref, nodes_ref, energy, cubes, packed, agg, corners,
):
    rows, ext, depth = v_ref.shape
    cx = rows // 3
    padded = energy.shape[1]
    groups = lane_groups(depth)
    n = lax.axis_index("narrow")
    w = lax.axis_index("wide")
    cy = (ext - 2 * RAD) // 3
    cols = 3 * cy
    reach = cy + 2

    even = lax.rem(w, 2) == 0
    valid = (jnp.where(n > 0, 1.0, 0.0), jnp.where(n < n_narrow - 1, 1.0, 0.0))
    for which, (one, other) in enumerate(((near_b, far_b), (near_a, far_a))):
        corners[which] = jnp.where(even, one[...], other[...]) * valid[which]
    for r in range(3):
        span = slice(r * cy, (r + 1) * cy)
        at = RAD * REACH + 2 * r
        for c in range(3):
            lanes = groups[c]
            for x in range(cx):
                nodes_ref[r, c, x] = nodes_in[r, c, x]
            nodes_ref[r, c, cx] = jnp.zeros_like(nodes_ref[r, c, cx])
            nodes_ref[r, c, cx, 1 : cy + 1, :] = jnp.where(even, near[RAD, span, lanes], row[span, lanes])
            nodes_ref[r, c, cx, 0:1, :] = corners[0, at + 1 : at + 2, lanes]
            nodes_ref[r, c, cx, cy + 1 : cy + 3, :] = corners[1, at : at + 2, lanes]
    lane = lax.broadcasted_iota(jnp.int32, nodes_ref.shape[3:], 1)
    for r in range(3):
        nodes = lambda c, x: nodes_ref[r, c, x]
        low = modes_of(nodes, 0, lane)
        for x in range(cx):
            high = modes_of(nodes, x + 1, lane)
            energy[r * cx + x] = element_energy(low, high)
            low = high

    recips = plane_reciprocals(n, n_narrow, cols, ext, depth)
    lows = low_ends()

    def coarse_row(x, carry):
        for sub in range(3):
            k = 3 * x + sub
            place_x = w * rows + k + jnp.zeros((8, LANES), jnp.int32)
            recip_x = reciprocal_weight(place_x, n_wide * rows)[0:1]

            def emit(r, g, lanes, gradient, cube):
                gg_ref[r, k, :, lanes] = gradient
                at = r * cx + x
                cubes[at, g] = cube if sub == 0 else cubes[at, g] + cube

            project_row(lambda lanes: v_ref[k, :, lanes], recip_x, recips, lows, emit, groups)
        return carry

    lax.fori_loop(0, cx, coarse_row, 0)

    agg[...] = element_sums(cubes, 3 * cx, packed, reach, padded)
    sub_id = lax.broadcasted_iota(jnp.int32, (padded, LANES), 0)
    keep = (sub_id > jnp.where(n > 0, -1, 0)) & (sub_id < reach)
    own = ((sub_id >= 1) & (sub_id <= cy)).astype(jnp.float32)
    part_ref[...] = jnp.zeros_like(part_ref)
    for r in range(3):
        partial = None
        for x in range(cx):
            at = r * cx + x
            value = modulus_of(agg[at * padded : (at + 1) * padded, :], r, keep)
            moduli_ref[at] = value
            term = value * energy[at]
            partial = term if partial is None else partial + term
        part_ref[r : r + 1, :] = jnp.sum(partial * own, axis=0, keepdims=True)


def nodal_rows(nodes, moduli, cx, first, lane):
    low = modes_of(nodes, first, lane)
    below = None
    for x in range(first, cx + 1):
        sums, above = None, None
        if x < cx:
            high = modes_of(nodes, x + 1, lane)
            forces = coupled_forces(element_modes(low, high))
            low = high
            modulus = moduli(x)
            scaled = [[None if f is None else modulus * f for f in mode] for mode in forces]
            sums = [[[None] * 3 for _ in range(2)] for _ in range(2)]
            above = [[[None] * 3 for _ in range(2)] for _ in range(2)]
            for my in range(2):
                for mz in range(2):
                    for comp in range(3):
                        even = scaled[2 * my + mz][comp]
                        odd = scaled[4 + 2 * my + mz][comp]
                        sums[my][mz][comp] = -odd if even is None else even - odd
                        above[my][mz][comp] = odd if even is None else even + odd
        yield x, sums, below
        below = above


def nodal_total(sums, below, comp, lane):
    along = []
    for mz in range(2):
        pair = []
        for my in range(2):
            terms = [part[my][mz][comp] for part in (sums, below) if part is not None]
            pair.append(terms[0] if len(terms) == 1 else terms[0] + terms[1])
        along.append((pair[0] - pair[1]) + pltpu.roll(pair[0] + pair[1], 1, 0))
    return (along[0] - along[1]) + jnp.where(
        lane >= 1, pltpu.roll(along[0] + along[1], 1, 1), 0.0
    )


def fields_kernel(
    n_wide, n_narrow, gg, energy, nodes_ref, near, far,
    summed_ref, extra_ref, moduli_ref, outer, spread_ref, packed, cubes, packed_outer,
):
    _, rows, ext, depth = gg.shape
    cx = rows // 3
    cols = 3 * ((ext - 2 * RAD) // 3)
    padded = energy.shape[1]
    reach = ext // 3
    groups = lane_groups(depth)
    n = lax.axis_index("narrow")
    w = lax.axis_index("wide")
    above = 1 - lax.rem(w, 2)
    row_id = lax.broadcasted_iota(jnp.int32, (LANES, LANES), 0)
    col_id = lax.broadcasted_iota(jnp.int32, (LANES, LANES), 1)
    coarse = cx + 2
    lane = lax.broadcasted_iota(jnp.int32, (padded, LANES), 1)
    for r in range(3):
        base = r * coarse
        for x in range(cx):
            packed[base + x + 1] = energy[r * cx + x]
        span = slice(RAD * ext + r * padded, RAD * ext + (r + 1) * padded)
        for c in range(3):
            extra_ref[r, c, above] = near[span, groups[c]]
            extra_ref[r, c, 1 - above] = far[span, groups[c]]
        first, last = (
            modes_of(lambda c, x: nodes_ref[r, c, x], x, lane) for x in (0, cx)
        )
        below, beyond = (
            modes_of(lambda c, x: extra_ref[r, c, x], x, lane) for x in (0, 1)
        )
        packed[base] = element_energy(below, first)
        packed[base + cx + 1] = element_energy(last, beyond)
    split = halves(packed[...].reshape(3 * coarse * padded, LANES))
    for g in range(len(groups)):
        copies = (row_id == (g * LANES + col_id) // 3).astype(jnp.float32).astype(jnp.bfloat16)
        fine = jnp.dot(
            split, jnp.concatenate([copies, copies], axis=0), preferred_element_type=jnp.float32
        )
        for at in range(3 * coarse):
            value = fine[at * padded : at * padded + reach]
            for sub in range(3):
                spread_ref[at, g, pl.ds(sub, reach, stride=3), :] = value
            if 3 * reach < ext:
                spread_ref[at, g, 3 * reach :, :] = jnp.zeros((ext - 3 * reach, LANES), jnp.float32)

    recips = plane_reciprocals(n, n_narrow, cols, ext, depth)
    lows = low_ends()

    def neighbour_row(k, carry):
        at = pl.multiple_of(k * ext, 8)
        for ref, side in ((near, above), (far, 1 - above)):
            first = w * rows + jnp.where(side == 0, -RAD, rows)
            place_x = first + k + jnp.zeros((8, LANES), jnp.int32)
            recip_x = reciprocal_weight(place_x, n_wide * rows)[0:1]

            def emit(r, g, lanes, gradient, cube):
                outer[r, side * RAD + k, :, lanes] = gradient
                cubes[k, side * 3 + r, g] = cube

            project_row(
                lambda lanes: ref[pl.ds(at, ext), lanes], recip_x, recips, lows, emit, groups
            )
        return carry

    lax.fori_loop(0, RAD, neighbour_row, 0)

    for r in range(3):
        for g in range(len(groups)):
            cubes[0, r, g] = cubes[0, r, g] + cubes[1, r, g] + cubes[2, r, g]
    sums = element_sums(cubes.at[0], 3, packed_outer, reach, padded)
    sub_id = lax.broadcasted_iota(jnp.int32, (padded, LANES), 0)
    last = jnp.where(w > 0, reach, 0)
    keep = (sub_id > jnp.where(n > 0, -1, 0)) & (sub_id < last)
    for r in range(3):
        moduli_ref[r] = modulus_of(sums[r * padded : (r + 1) * padded], r, keep)

    for r in range(3):
        def first_dim(s, carry):
            place = pl.ds(pl.multiple_of(8 * s, 8), 8)
            for g, lanes in enumerate(groups):
                column = []
                for x in range(coarse):
                    spread = spread_ref[r * coarse + x, g, place, :]
                    for sub in range(3):
                        if x == 0:
                            value = outer[r, sub, place, lanes]
                        elif x == coarse - 1:
                            value = outer[r, RAD + sub, place, lanes]
                        else:
                            value = gg[r, 3 * (x - 1) + sub, place, lanes]
                        column.append(value * spread)
                for k, value in enumerate(tent_rows(column)):
                    summed_ref[r, k, place, lanes] = value
            return carry

        lax.fori_loop(0, ext // 8, first_dim, 0)


def force_kernel(nodes_ref, extra, moduli, moduli_below, support, loading, residual_ref):
    cx, cy, _ = support.shape
    lane = lax.broadcasted_iota(jnp.int32, nodes_ref.shape[3:], 1)
    for r in range(3):
        nodes = lambda c, x: extra[r, c, 0] if x < 0 else nodes_ref[r, c, x]
        modulus = lambda x: moduli_below[r] if x < 0 else moduli[r * cx + x]
        for x, sums, below in nodal_rows(nodes, modulus, cx, -1, lane):
            if 0 <= x < cx:
                free = 1.0 - support[x].astype(jnp.float32)
                for comp in range(3):
                    total = nodal_total(sums, below, comp, lane)[1 : cy + 1]
                    if comp == 2:
                        total = total + load_force * loading[x].astype(jnp.float32)
                    residual_ref[r, comp, x] = -total * free


def realization_factors(part, shape):
    factors, totals = [], []
    for r in range(3):
        total = jnp.sum(part[r : r + 1, :], axis=1, keepdims=True)
        factor = 3.0 * (1.0 - stiff_floor) / 27.0 * sharpness / DENOM[r] ** 3
        factors.append(jnp.broadcast_to(-factor / total, shape))
        totals.append(total)
    return factors, totals


def final_kernel(part, summed, out_ref, compliance_ref):
    rows, cols, depth = out_ref.shape
    groups = lane_groups(depth)
    factors, totals = realization_factors(part, (1, LANES))
    for r in range(3):
        compliance_ref[r] = jnp.sum(totals[r])

    def other_dims(step, carry):
        for sub in range(3):
            k = 3 * step + sub
            parts = []
            for lanes in groups:
                total = None
                for r in range(3):
                    term = factors[r] * summed[r, k, :, lanes]
                    total = term if total is None else total + term
                parts.append(tent_sublanes(total, cols))
            for lanes, value in zip(groups, tent_lanes(parts)):
                out_ref[k, :, lanes] = value
        return carry

    for step in range(rows // 3):
        other_dims(step, 0)


def call(kernel, shapes, scratch, flops, args, hbm=0, scalars=(), limit=20):
    vmem = pl.BlockSpec(memory_space=pltpu.VMEM)
    smem = pl.BlockSpec(memory_space=pltpu.SMEM)
    scratch = [pltpu.VMEM(s, jnp.float32) if isinstance(s, tuple) else s for s in scratch]
    args = [
        pltpu.with_memory_space_constraint(arg, pltpu.HBM) if i < hbm else arg
        for i, arg in enumerate(args)
    ]
    return pl.pallas_call(
        kernel,
        out_shape=[jax.ShapeDtypeStruct(s, jnp.float32) for s in list(shapes) + list(scalars)],
        in_specs=[pl.BlockSpec(memory_space=pltpu.HBM)] * hbm + [vmem] * (len(args) - hbm),
        out_specs=[vmem] * len(shapes) + [smem] * len(scalars),
        scratch_shapes=scratch,
        compiler_params=pltpu.CompilerParams(vmem_limit_bytes=limit * 1024 * 1024),
        cost_estimate=pl.CostEstimate(flops=flops, bytes_accessed=1000000, transcendentals=0),
    )(*args)


def ceil8(amount):
    return -(-amount // 8) * 8


def exchange_sum(value, total, group):
    axes = ("wide", "narrow")
    parts = [lax.ppermute(value, axes, [(i, i ^ k) for i in range(total)]) for k in group]
    for part in parts:
        value = value + part
    return value


def local(n_wide, n_narrow, design, passive, displacement, support, loading):
    rows, cols, depth = design.shape
    cx, cy, cz = support.shape
    merged = n_narrow == 2
    axes = ("wide", "narrow")
    ext = ceil8(cols + 2 * RAD)
    padded = ceil8(cy + 3)

    def route(toward, dy):
        pairs = []
        for i in range(n_wide):
            if toward == "down" and i % 2:
                continue
            mate = {"near": i ^ 1, "far": i + 1 if i % 2 else i - 1, "self": i, "down": i - 1}[toward]
            for j in range(n_narrow):
                if 0 <= mate < n_wide and 0 <= j + dy < n_narrow:
                    pairs.append((i * n_narrow + j, mate * n_narrow + j + dy))
        return pairs

    def side_route(toward, index):
        if merged:
            return route(toward, 1) + route(toward, -1)
        return route(toward, 1 if index == 0 else -1)

    def send(block, pairs):
        return lax.ppermute(block, axes, pairs)

    kinds = ("merged",) if merged else ("high", "low")
    sides = len(kinds)
    corner = (ceil8(RAD * REACH + 6), depth)
    ends = (RAD, cols, depth)
    nodes_shape = (3, 3, cx, padded, cz)
    coarse_shape = (3 * cx, padded, cz)
    count = ceil8(cols + 2 * REACH)
    ints = lambda *shape: pltpu.VMEM(shape, jnp.int32)
    packs = call(
        functools.partial(pack_kernel, kinds),
        [(RAD + 1, cols, depth), ends, (3 * cy, depth), nodes_shape]
        + [(ceil8(rows * (REACH + RAD) + 6 * cx), depth), corner, corner] * sides,
        [
            (sides, rows, 8, depth), ints(sides, rows, 8, depth), displacement.shape,
            ints(*support.shape), pltpu.SemaphoreType.DMA((4 + 2 * sides,)),
        ],
        200000, (design, passive, displacement, support), hbm=4,
    )
    far = send(packs[1], route("far", 0))
    got = []
    for index in range(sides):
        side, side_near, side_far = packs[4 + 3 * index : 7 + 3 * index]
        got.append((
            send(side, side_route("self", index)),
            send(side_near, side_route("near", index)),
            send(side_far, side_route("far", index)),
        ))
    near = send(packs[0], route("near", 0))
    row = send(packs[2], route("down", 0))
    own_design, own_mask = call(
        load_kernel, [design.shape, (rows, ext, depth)],
        [ints(*passive.shape), pltpu.SemaphoreType.DMA((2,))],
        200000, (design, passive), hbm=2,
    )
    before, after = got[0], got[-1]
    corners = (before[1], after[1], before[2], after[2])
    outer = (RAD * ext + 3 * padded, depth)
    v, nodes, v_near, v_far = call(
        functools.partial(blur_kernel, n_wide, n_narrow),
        [(rows, ext, depth), nodes_shape, outer, outer],
        [(2,) + ends, (2, 2) + corner, (rows, count, depth), (rows, ext, depth)],
        10000000,
        (own_design, own_mask, packs[3], near, far, before[0], after[0]) + corners,
    )
    v_far = send(v_far, route("far", 0))
    v_near = send(v_near, route("near", 0))
    gg, moduli, part, nodes, energy = call(
        functools.partial(project_kernel, n_wide, n_narrow),
        [
            (3, rows, ext, depth), coarse_shape, (8, LANES), (3, 3, cx + 1, padded, cz),
            coarse_shape,
        ],
        [
            (3 * cx, depth // LANES, ext, LANES), (3 * cx * padded, LANES),
            (3 * cx * padded, LANES), (2,) + corner,
        ],
        10000000, (v, nodes, near, row) + corners,
    )
    total = n_wide * n_narrow
    steps = [1 << bit for bit in range(total.bit_length() - 1)]
    groups = [(s,) for s in steps[:-2]] + [(steps[-2], steps[-1], steps[-2] + steps[-1])]
    fields, extra, moduli_below = call(
        functools.partial(fields_kernel, n_wide, n_narrow),
        [(3, rows, ext, depth), (3, 3, 2, padded, cz), (3, padded, cz)],
        [
            (3, 2 * RAD, ext, depth), (3 * (cx + 2), depth // LANES, ext, LANES),
            (3 * (cx + 2), padded, LANES), (RAD, 6, depth // LANES, ext, LANES),
            (3 * padded, LANES),
        ],
        10000000, (gg, energy, nodes, v_near, v_far),
    )
    (residual,) = call(
        force_kernel, [displacement.shape], [], 10000000,
        (nodes, extra, moduli, moduli_below, support, loading),
    )
    summed = part
    for group in groups:
        summed = exchange_sum(summed, total, group)
    sensitivity, compliance = call(
        final_kernel, [design.shape], [], 10000000, (summed, fields), scalars=[(3,)],
    )
    return residual, compliance, sensitivity


def solution(mesh):
    in_specs = (
        P("wide", "narrow", None),
        P("wide", "narrow", None),
        P(None, None, "wide", "narrow", None),
        P("wide", "narrow", None),
        P("wide", "narrow", None),
    )
    out_specs = (P(None, None, "wide", "narrow", None), P(), P("wide", "narrow", None))

    def body(*args):
        return local(mesh.shape["wide"], mesh.shape["narrow"], *args)

    return jax.shard_map(body, mesh=mesh, in_specs=in_specs, out_specs=out_specs, check_vma=False)
```

```python
import functools
import math

import jax
import jax.numpy as jnp
import numpy as np
from jax import lax
from jax.experimental import pallas as pl
from jax.experimental.pallas import tpu as pltpu
from jax.sharding import PartitionSpec as P


RAD = 3
sharpness = 8.0
thresholds = (0.7, 0.5, 0.3)
stiff_floor = 0.001
load_force = 4.0
poisson = 0.3
LANES = 128
REACH = 2 * RAD


def element_matrix():
    inv_root = 1.0 / np.sqrt(3.0)
    elastic_scale = 1.0 / ((1.0 + poisson) * (1.0 - 2.0 * poisson))
    elastic = np.zeros((6, 6))
    for row_i in range(3):
        for col_j in range(3):
            elastic[row_i, col_j] = poisson
        elastic[row_i, row_i] = 1.0 - poisson
    for row_i in range(3, 6):
        elastic[row_i, row_i] = 0.5 - poisson
    elastic = elastic * elastic_scale
    corner_signs = [
        (2 * (corner // 4) - 1, 2 * (corner // 2 % 2) - 1, 2 * (corner % 2) - 1)
        for corner in range(8)
    ]
    stiffness = np.zeros((24, 24))
    for gauss_a in (-inv_root, inv_root):
        for gauss_b in (-inv_root, inv_root):
            for gauss_c in (-inv_root, inv_root):
                gauss_point = (gauss_a, gauss_b, gauss_c)
                derivs = np.zeros((8, 3))
                for corner in range(8):
                    for along in range(3):
                        slope_value = corner_signs[corner][along] / 8.0
                        for second in range(3):
                            if second != along:
                                slope_value = slope_value * (
                                    1.0 + corner_signs[corner][second] * gauss_point[second]
                                )
                        derivs[corner, along] = 2.0 * slope_value
                strain = np.zeros((6, 24))
                for corner in range(8):
                    column = 3 * corner
                    strain[0, column] = derivs[corner, 0]
                    strain[1, column + 1] = derivs[corner, 1]
                    strain[2, column + 2] = derivs[corner, 2]
                    strain[3, column] = derivs[corner, 1]
                    strain[3, column + 1] = derivs[corner, 0]
                    strain[4, column + 1] = derivs[corner, 2]
                    strain[4, column + 2] = derivs[corner, 1]
                    strain[5, column] = derivs[corner, 2]
                    strain[5, column + 2] = derivs[corner, 0]
                stiffness = stiffness + strain.T @ elastic @ strain * 0.125
    return stiffness


def parity_operator():
    signs = np.ones((8, 8))
    for mode in range(8):
        for corner in range(8):
            for bit in range(3):
                if (mode >> bit) & 1:
                    signs[mode, corner] *= 2 * ((corner >> bit) & 1) - 1
    full = np.kron(signs, np.eye(3))
    coupled = full @ element_matrix() @ full.T / 64.0
    coupled[np.abs(coupled) < 1e-9] = 0.0
    return coupled


COUPLED = parity_operator()
LOW_END = tuple(math.tanh(sharpness * eta) for eta in thresholds)
DENOM = tuple(
    math.tanh(sharpness * eta) + math.tanh(sharpness * (1.0 - eta)) for eta in thresholds
)


def tent_rows(rows):
    for step in (1, 2, 1, 2):
        rows = [rows[i] + rows[i + step] for i in range(len(rows) - step)]
    return rows


def tent_sublanes(block, amount):
    size = block.shape[0]
    for step in (1, 2, 1, 2):
        block = block + pltpu.roll(block, size - step, 0)
    return block[:amount]


def lanes_up(parts, step, lane):
    rolled = [pltpu.roll(part, LANES - step, 1) for part in parts]
    rolled.append(jnp.zeros_like(parts[0]))
    return [
        jnp.where(lane < LANES - step, rolled[g], rolled[g + 1]) for g in range(len(parts))
    ]


def lanes_down(parts, step, lane):
    rolled = [jnp.zeros_like(parts[0])] + [pltpu.roll(part, step, 1) for part in parts]
    return [jnp.where(lane >= step, rolled[g + 1], rolled[g]) for g in range(len(parts))]


def tent_lanes(parts):
    lane = lax.broadcasted_iota(jnp.int32, parts[0].shape, 1)
    total = [4.0 * part for part in parts]
    for step in range(1, RAD + 1):
        ups, downs = lanes_up(parts, step, lane), lanes_down(parts, step, lane)
        if step == RAD:
            total = [t + (u + d) for t, u, d in zip(total, ups, downs)]
        else:
            total = [
                t + float(RAD + 1 - step) * (u + d) for t, u, d in zip(total, ups, downs)
            ]
    return total


def tent_weight(place, extent):
    total = jnp.zeros(place.shape, jnp.float32)
    for offset in range(-RAD, RAD + 1):
        inside = (place + offset >= 0) & (place + offset < extent)
        total = total + jnp.where(inside, float(RAD + 1 - abs(offset)), 0.0)
    return total


def halves(block):
    high = block.astype(jnp.bfloat16)
    low = (block - high.astype(jnp.float32)).astype(jnp.bfloat16)
    return jnp.concatenate([high, low], axis=1)


def lane_groups(depth):
    return [slice(g * LANES, (g + 1) * LANES) for g in range(depth // LANES)]


def modes_of(nodes, row, lane):
    fields = [[[None] * 3 for _ in range(2)] for _ in range(2)]
    for comp in range(3):
        value = nodes(comp, row)
        size = value.shape[0]
        ahead = jnp.where(lane < LANES - 1, pltpu.roll(value, LANES - 1, 1), 0.0)
        for mz, part in enumerate((value + ahead, ahead - value)):
            beside = pltpu.roll(part, size - 1, 0)
            fields[0][mz][comp] = part + beside
            fields[1][mz][comp] = beside - part
    return fields


def element_modes(low, high):
    modes = []
    for mx in range(2):
        for my in range(2):
            for mz in range(2):
                modes.append([
                    (h + l) if mx == 0 else (h - l)
                    for l, h in zip(low[my][mz], high[my][mz])
                ])
    return modes


def coupled_forces(modes):
    forces = [[None] * 3 for _ in range(8)]
    for mode in range(8):
        for comp in range(3):
            row = COUPLED[3 * mode + comp]
            groups = {}
            for place in np.nonzero(row)[0]:
                groups.setdefault(round(float(row[place]), 12), []).append(int(place))
            total = None
            for factor, places in groups.items():
                summed = modes[places[0] // 3][places[0] % 3]
                for place in places[1:]:
                    summed = summed + modes[place // 3][place % 3]
                term = factor * summed
                total = term if total is None else total + term
            forces[mode][comp] = total
    return forces


def pick(n, high, low, kind):
    if kind == "merged":
        return jnp.where(n == 0, high, low)
    return high if kind == "high" else low


def column_start(n, cols, kind):
    if kind == "merged":
        return pl.multiple_of(jnp.where(n == 0, cols - 8, 0), 8)
    return cols - 8 if kind == "high" else 0


def fill_tail(ref, used):
    if ref.shape[0] > used:
        ref[used:, :] = jnp.zeros((ref.shape[0] - used, ref.shape[1]), jnp.float32)


def pack_kernel(
    kinds, design, passive, disp, support, near_ref, far_ref, row_ref, nodes_ref, *rest
):
    rows, cols, depth = design.shape
    cx, cy, _ = support.shape
    sides, (edges, masks, moves, frees, sems) = rest[: 2 * len(kinds)], rest[2 * len(kinds) :]
    groups = lane_groups(depth)
    n = lax.axis_index("narrow")
    even = lax.rem(lax.axis_index("wide"), 2) == 0
    near_start = jnp.where(even, rows - RAD, 0)
    far_start = jnp.where(even, 0, rows - RAD)
    copies = [
        pltpu.make_async_copy(disp, moves, sems.at[0]),
        pltpu.make_async_copy(support, frees, sems.at[1]),
    ]
    for index, kind in enumerate(kinds):
        start = column_start(n, cols, kind)
        copies.append(
            pltpu.make_async_copy(
                design.at[:, pl.ds(start, 8), :], edges.at[index], sems.at[2 + 2 * index]
            )
        )
        copies.append(
            pltpu.make_async_copy(
                passive.at[:, pl.ds(start, 8), :], masks.at[index], sems.at[3 + 2 * index]
            )
        )
    last = 2 + 2 * len(kinds)
    for at, start, ref in ((last, near_start, near_ref), (last + 1, far_start, far_ref)):
        copies.append(
            pltpu.make_async_copy(design.at[pl.ds(start, RAD)], ref.at[:RAD], sems.at[at])
        )
    for copy in copies:
        copy.start()
    nodes_ref[...] = jnp.zeros_like(nodes_ref)
    for copy in copies[:2]:
        copy.wait()
    for x in range(cx):
        free = 1.0 - frees[x].astype(jnp.float32)
        for r in range(3):
            for c in range(3):
                value = moves[r, c, x] * free
                nodes_ref[r, c, x, 1 : cy + 1, :] = value
                if x == 0:
                    near_ref[RAD, r * cy : (r + 1) * cy, groups[c]] = value
                    row_ref[r * cy : (r + 1) * cy, groups[c]] = value
    for copy in copies[2:last]:
        copy.wait()

    for index, kind in enumerate(kinds):
        side, side_far = sides[2 * index : 2 * index + 2]
        for k in range(rows):
            value = edges[index, k]
            piece = pick(n, value[8 - REACH :], value[:REACH], kind)
            side[pl.ds(k * REACH, REACH), :] = piece
            value = 1.0 - masks[index, k].astype(jnp.float32)
            side[pl.ds(rows * REACH + k * RAD, RAD), :] = pick(n, value[8 - RAD :], value[:RAD], kind)
        for k in range(RAD):
            value = edges[index, far_start + k]
            piece = pick(n, value[8 - REACH :], value[:REACH], kind)
            side_far[pl.ds(k * REACH, REACH), :] = piece
        base = rows * (REACH + RAD)
        for r in range(3):
            for c in range(3):
                for x in range(cx):
                    value = nodes_ref[r, c, x]
                    piece = pick(n, value[cy - 1 : cy + 1], value[1:3], kind)
                    side[pl.ds(base + (r * cx + x) * 2, 2), groups[c]] = piece
                    if x == 0:
                        side_far[pl.ds(RAD * REACH + 2 * r, 2), groups[c]] = piece
        fill_tail(side, base + 6 * cx)
        fill_tail(side_far, RAD * REACH + 6)
    for copy in copies[last:]:
        copy.wait()


def element_energy(low, high):
    modes = element_modes(low, high)
    forces = coupled_forces(modes)
    total = None
    for mode in range(8):
        for comp in range(3):
            if forces[mode][comp] is not None:
                term = modes[mode][comp] * forces[mode][comp]
                total = term if total is None else total + term
    return total


def reciprocal_weight(place, extent):
    inside = (place >= 0) & (place < extent)
    return jnp.where(inside, 1.0 / jnp.maximum(tent_weight(place, extent), 1.0), 0.0)


def plane_reciprocals(n, n_narrow, cols, ext, depth):
    place_y = n * cols - RAD + lax.broadcasted_iota(jnp.int32, (ext, LANES), 0)
    recip_y = reciprocal_weight(place_y, n_narrow * cols)
    recip_z = []
    for g in range(depth // LANES):
        place_z = g * LANES + lax.broadcasted_iota(jnp.int32, (ext, LANES), 1)
        recip_z.append(1.0 / tent_weight(place_z, depth))
    return recip_y, recip_z


def low_ends():
    return [jnp.tanh(jnp.full((1, LANES), sharpness * eta, jnp.float32)) for eta in thresholds]


def project_row(row, recip_x, recips, lows, emit, groups):
    recip_y, recip_z = recips
    recip_xy = recip_y * recip_x
    for g, lanes in enumerate(groups):
        recip = recip_xy * recip_z[g]
        scaled = sharpness * row(lanes)
        for r in range(3):
            steep = jnp.tanh(scaled - sharpness * thresholds[r])
            dense = steep + lows[r]
            square = dense * dense
            emit(r, g, lanes, square * (1.0 - steep * steep) * recip, square * dense)


def element_sums(cubes, amount, packed, reach, padded):
    row_id = lax.broadcasted_iota(jnp.int32, (LANES, LANES), 0)
    col_id = lax.broadcasted_iota(jnp.int32, (LANES, LANES), 1)
    total = None
    packed[...] = jnp.zeros_like(packed)
    for g in range(cubes.shape[1]):
        for at in range(amount):
            summed = cubes[at, g, pl.ds(0, reach, stride=3), :]
            summed = summed + cubes[at, g, pl.ds(1, reach, stride=3), :]
            summed = summed + cubes[at, g, pl.ds(2, reach, stride=3), :]
            packed[at * padded : at * padded + reach, :] = summed
        gather = ((g * LANES + row_id) // 3 == col_id).astype(jnp.float32).astype(jnp.bfloat16)
        term = jnp.dot(
            halves(packed[...]),
            jnp.concatenate([gather, gather], axis=0),
            preferred_element_type=jnp.float32,
        )
        total = term if total is None else total + term
    return total


def modulus_of(value, r, keep):
    value = stiff_floor + ((1.0 - stiff_floor) / 27.0 / DENOM[r] ** 3) * value
    return jnp.where(keep, value, 0.0)


def load_kernel(design_hbm, passive_hbm, design, mask_ref, passive, sems):
    rows, cols, depth = design.shape
    copies = [
        pltpu.make_async_copy(passive_hbm, passive, sems.at[0]),
        pltpu.make_async_copy(design_hbm, design, sems.at[1]),
    ]
    for copy in copies:
        copy.start()
    copies[0].wait()
    for k in range(rows):
        mask_ref[k, RAD : RAD + cols, :] = 1.0 - passive[k].astype(jnp.float32)
        mask_ref[k, :RAD, :] = jnp.zeros((RAD, depth), jnp.float32)
        tail = mask_ref.shape[1] - RAD - cols
        mask_ref[k, RAD + cols :, :] = jnp.zeros((tail, depth), jnp.float32)
    copies[1].wait()


def blur_kernel(
    n_wide, n_narrow, design, mask_in, nodes_in, near, far,
    side_b, side_a, near_b, near_a, far_b, far_a,
    v_ref, nodes_ref, near_ref, far_ref, ends, corners, blurred, edge_mask,
):
    rows, cols, depth = design.shape
    cx = nodes_ref.shape[2]
    cy = cols // 3
    groups = lane_groups(depth)
    n = lax.axis_index("narrow")
    w = lax.axis_index("wide")
    valid_b = jnp.where(n > 0, 1.0, 0.0)
    valid_a = jnp.where(n < n_narrow - 1, 1.0, 0.0)
    ext = v_ref.shape[1]

    above = 1 - lax.rem(w, 2)
    for index, ref in ((above, near), (1 - above, far)):
        for k in range(RAD):
            ends[index, k] = ref[k]
    reach = RAD * REACH
    last = (rows - RAD) * REACH
    for which, (one, other) in enumerate(((near_b, far_b), (near_a, far_a))):
        valid = (valid_b, valid_a)[which]
        piece = jnp.where(above == 1, one[:reach], one[last : last + reach])
        corners[which, above, :reach] = piece * valid
        corners[which, 1 - above, :reach] = other[:reach] * valid

    base = rows * (REACH + RAD)
    for r in range(3):
        for c in range(3):
            lanes = groups[c]
            for x in range(cx):
                nodes_ref[r, c, x] = nodes_in[r, c, x]
                at = base + (r * cx + x) * 2
                nodes_ref[r, c, x, 0:1, :] = side_b[at + 1 : at + 2, lanes] * valid_b
                nodes_ref[r, c, x, cy + 1 : cy + 3, :] = side_a[at : at + 2, lanes] * valid_a

    for start in range(0, cols, 8):
        place = slice(start, start + 8)
        for lanes in groups:
            column = [ends[0, k, place, lanes] for k in range(RAD)]
            column += [design[k, place, lanes] for k in range(rows)]
            column += [ends[1, k, place, lanes] for k in range(RAD)]
            for k, value in enumerate(tent_rows(column)):
                blurred[k, REACH + start : REACH + start + 8, lanes] = value
    span = lambda k: slice(k * REACH, (k + 1) * REACH)
    for which, at, side, valid in ((0, 0, side_b, valid_b), (1, REACH + cols, side_a, valid_a)):
        for lanes in groups:
            column = [corners[which, 0, span(k), lanes] for k in range(RAD)]
            column += [side[span(k), lanes] * valid for k in range(rows)]
            column += [corners[which, 1, span(k), lanes] for k in range(RAD)]
            for k, value in enumerate(tent_rows(column)):
                blurred[k, at : at + REACH, lanes] = value
    tail = blurred.shape[1] - cols - 2 * REACH
    if tail:
        blurred[:, cols + 2 * REACH :, :] = jnp.zeros((rows, tail, depth), jnp.float32)

    edge_mask[...] = mask_in[...]
    for k in range(rows):
        at = rows * REACH + k * RAD
        edge_mask[k, 0:RAD, :] = side_b[at : at + RAD, :]
        edge_mask[k, RAD + cols : 2 * RAD + cols, :] = side_a[at : at + RAD, :]

    recip_y, recip_z = plane_reciprocals(n, n_narrow, cols, ext, depth)

    def fine_row(x, carry):
        for sub in range(3):
            k = 3 * x + sub
            parts = tent_lanes([tent_sublanes(blurred[k, :, lanes], ext) for lanes in groups])
            place_x = w * rows + k + jnp.zeros((8, LANES), jnp.int32)
            recip_x = reciprocal_weight(place_x, n_wide * rows)[0:1]
            recip_xy = recip_y * recip_x
            for g, lanes in enumerate(groups):
                v_ref[k, :, lanes] = (recip_xy * recip_z[g]) * parts[g] * edge_mask[k, :, lanes]
        return carry

    for x in range(cx):
        fine_row(x, 0)

    near_first, near_x = above * (rows - RAD), 1 + above * (cx - 2)
    for ref, first, x in (
        (near_ref, near_first, near_x), (far_ref, rows - RAD - near_first, cx - near_x)
    ):
        for k in range(RAD):
            ref[k * ext : (k + 1) * ext, :] = v_ref[first + k]
        for r in range(3):
            at = RAD * ext + r * nodes_ref.shape[3]
            for c in range(3):
                ref[at : at + nodes_ref.shape[3], groups[c]] = nodes_ref[r, c, x]


def project_kernel(
    n_wide, n_narrow, v_ref, nodes_in, near, row, near_b, near_a, far_b, far_a,
    gg_ref, moduli_ref, part_ref, nodes_ref, energy, cubes, packed, agg, corners,
):
    rows, ext, depth = v_ref.shape
    cx = rows // 3
    padded = energy.shape[1]
    groups = lane_groups(depth)
    n = lax.axis_index("narrow")
    w = lax.axis_index("wide")
    cy = (ext - 2 * RAD) // 3
    cols = 3 * cy
    reach = cy + 2

    even = lax.rem(w, 2) == 0
    valid = (jnp.where(n > 0, 1.0, 0.0), jnp.where(n < n_narrow - 1, 1.0, 0.0))
    for which, (one, other) in enumerate(((near_b, far_b), (near_a, far_a))):
        for r in range(3):
            here = rows * (REACH + RAD) + r * cx * 2
            there = RAD * REACH + 2 * r
            piece = jnp.where(even, one[here : here + 2], other[there : there + 2])
            corners[which, 2 * r : 2 * r + 2] = piece * valid[which]
    for r in range(3):
        span = slice(r * cy, (r + 1) * cy)
        at = 2 * r
        for c in range(3):
            lanes = groups[c]
            for x in range(cx):
                nodes_ref[r, c, x] = nodes_in[r, c, x]
            nodes_ref[r, c, cx] = jnp.zeros_like(nodes_ref[r, c, cx])
            nodes_ref[r, c, cx, 1 : cy + 1, :] = jnp.where(even, near[RAD, span, lanes], row[span, lanes])
            nodes_ref[r, c, cx, 0:1, :] = corners[0, at + 1 : at + 2, lanes]
            nodes_ref[r, c, cx, cy + 1 : cy + 3, :] = corners[1, at : at + 2, lanes]
    lane = lax.broadcasted_iota(jnp.int32, nodes_ref.shape[3:], 1)
    for r in range(3):
        nodes = lambda c, x: nodes_ref[r, c, x]
        low = modes_of(nodes, 0, lane)
        for x in range(cx):
            high = modes_of(nodes, x + 1, lane)
            energy[r * cx + x] = element_energy(low, high)
            low = high

    recips = plane_reciprocals(n, n_narrow, cols, ext, depth)
    lows = low_ends()

    def coarse_row(x, carry):
        for sub in range(3):
            k = 3 * x + sub
            place_x = w * rows + k + jnp.zeros((8, LANES), jnp.int32)
            recip_x = reciprocal_weight(place_x, n_wide * rows)[0:1]

            def emit(r, g, lanes, gradient, cube):
                gg_ref[r, k, :, lanes] = gradient
                at = r * cx + x
                cubes[at, g] = cube if sub == 0 else cubes[at, g] + cube

            project_row(lambda lanes: v_ref[k, :, lanes], recip_x, recips, lows, emit, groups)
        return carry

    lax.fori_loop(0, cx, coarse_row, 0)

    agg[...] = element_sums(cubes, 3 * cx, packed, reach, padded)
    sub_id = lax.broadcasted_iota(jnp.int32, (padded, LANES), 0)
    keep = (sub_id > jnp.where(n > 0, -1, 0)) & (sub_id < reach)
    own = ((sub_id >= 1) & (sub_id <= cy)).astype(jnp.float32)
    part_ref[...] = jnp.zeros_like(part_ref)
    for r in range(3):
        partial = None
        for x in range(cx):
            at = r * cx + x
            value = modulus_of(agg[at * padded : (at + 1) * padded, :], r, keep)
            moduli_ref[at] = value
            term = value * energy[at]
            partial = term if partial is None else partial + term
        summed = jnp.sum(jnp.sum(partial * own, axis=0, keepdims=True), axis=1, keepdims=True)
        part_ref[r : r + 1, :] = jnp.broadcast_to(summed, (1, LANES))


def nodal_rows(nodes, moduli, cx, first, lane):
    low = modes_of(nodes, first, lane)
    below = None
    for x in range(first, cx + 1):
        sums, above = None, None
        if x < cx:
            high = modes_of(nodes, x + 1, lane)
            forces = coupled_forces(element_modes(low, high))
            low = high
            modulus = moduli(x)
            scaled = [[None if f is None else modulus * f for f in mode] for mode in forces]
            sums = [[[None] * 3 for _ in range(2)] for _ in range(2)]
            above = [[[None] * 3 for _ in range(2)] for _ in range(2)]
            for my in range(2):
                for mz in range(2):
                    for comp in range(3):
                        even = scaled[2 * my + mz][comp]
                        odd = scaled[4 + 2 * my + mz][comp]
                        sums[my][mz][comp] = -odd if even is None else even - odd
                        above[my][mz][comp] = odd if even is None else even + odd
        yield x, sums, below
        below = above


def nodal_total(sums, below, comp, lane):
    along = []
    for mz in range(2):
        pair = []
        for my in range(2):
            terms = [part[my][mz][comp] for part in (sums, below) if part is not None]
            pair.append(terms[0] if len(terms) == 1 else terms[0] + terms[1])
        along.append((pair[0] - pair[1]) + pltpu.roll(pair[0] + pair[1], 1, 0))
    return (along[0] - along[1]) + jnp.where(
        lane >= 1, pltpu.roll(along[0] + along[1], 1, 1), 0.0
    )


def outer_kernel(
    n_wide, n_narrow, energy, nodes_ref, near, far,
    outer, spread_ref, force_ref, extra_ref, packed, cubes, packed_outer,
):
    _, _, ext, depth = outer.shape
    cx = nodes_ref.shape[2] - 1
    rows = 3 * cx
    cols = 3 * ((ext - 2 * RAD) // 3)
    padded = energy.shape[1]
    reach = ext // 3
    groups = lane_groups(depth)
    n = lax.axis_index("narrow")
    w = lax.axis_index("wide")
    above = 1 - lax.rem(w, 2)
    row_id = lax.broadcasted_iota(jnp.int32, (LANES, LANES), 0)
    col_id = lax.broadcasted_iota(jnp.int32, (LANES, LANES), 1)
    coarse = cx + 2
    lane = lax.broadcasted_iota(jnp.int32, (padded, LANES), 1)
    for r in range(3):
        base = r * coarse
        for x in range(cx):
            packed[base + x + 1] = energy[r * cx + x]
        span = slice(RAD * ext + r * padded, RAD * ext + (r + 1) * padded)
        for c in range(3):
            extra_ref[r, c, above] = near[span, groups[c]]
            extra_ref[r, c, 1 - above] = far[span, groups[c]]
        first, last = (
            modes_of(lambda c, x: nodes_ref[r, c, x], x, lane) for x in (0, cx)
        )
        below, beyond = (
            modes_of(lambda c, x: extra_ref[r, c, x], x, lane) for x in (0, 1)
        )
        packed[base] = element_energy(below, first)
        packed[base + cx + 1] = element_energy(last, beyond)
    split = halves(packed[...].reshape(3 * coarse * padded, LANES))
    for g in range(len(groups)):
        copies = (row_id == (g * LANES + col_id) // 3).astype(jnp.float32).astype(jnp.bfloat16)
        fine = jnp.dot(
            split, jnp.concatenate([copies, copies], axis=0), preferred_element_type=jnp.float32
        )
        for at in range(3 * coarse):
            value = fine[at * padded : at * padded + reach]
            for sub in range(3):
                spread_ref[at, g, pl.ds(sub, reach, stride=3), :] = value
            if 3 * reach < ext:
                spread_ref[at, g, 3 * reach :, :] = jnp.zeros((ext - 3 * reach, LANES), jnp.float32)

    recips = plane_reciprocals(n, n_narrow, cols, ext, depth)
    lows = low_ends()

    def neighbour_row(k, carry):
        at = pl.multiple_of(k * ext, 8)
        for ref, side in ((near, above), (far, 1 - above)):
            first = w * rows + jnp.where(side == 0, -RAD, rows)
            place_x = first + k + jnp.zeros((8, LANES), jnp.int32)
            recip_x = reciprocal_weight(place_x, n_wide * rows)[0:1]

            def emit(r, g, lanes, gradient, cube):
                outer[r, side * RAD + k, :, lanes] = gradient
                cubes[k, side * 3 + r, g] = cube

            project_row(
                lambda lanes: ref[pl.ds(at, ext), lanes], recip_x, recips, lows, emit, groups
            )
        return carry

    lax.fori_loop(0, RAD, neighbour_row, 0)

    for r in range(3):
        for g in range(len(groups)):
            cubes[0, r, g] = cubes[0, r, g] + cubes[1, r, g] + cubes[2, r, g]
    sums = element_sums(cubes.at[0], 3, packed_outer, reach, padded)
    sub_id = lax.broadcasted_iota(jnp.int32, (padded, LANES), 0)
    last = jnp.where(w > 0, reach, 0)
    keep = (sub_id > jnp.where(n > 0, -1, 0)) & (sub_id < last)
    cy = cols // 3
    for r in range(3):
        modulus = modulus_of(sums[r * padded : (r + 1) * padded], r, keep)
        nodes = lambda c, x: extra_ref[r, c, 0] if x < 0 else nodes_ref[r, c, x]
        for x, sums_at, below in nodal_rows(nodes, lambda x: modulus, 0, -1, lane):
            if x == 0:
                for comp in range(3):
                    total = nodal_total(sums_at, below, comp, lane)
                    force_ref[r, comp] = total[1 : cy + 1]


def fields_kernel(gg, outer, spread_ref, summed_ref):
    _, rows, ext, depth = gg.shape
    coarse = rows // 3 + 2
    groups = lane_groups(depth)
    for r in range(3):
        def first_dim(s, carry):
            place = pl.ds(pl.multiple_of(8 * s, 8), 8)
            for g, lanes in enumerate(groups):
                column = []
                for x in range(coarse):
                    spread = spread_ref[r * coarse + x, g, place, :]
                    for sub in range(3):
                        if x == 0:
                            value = outer[r, sub, place, lanes]
                        elif x == coarse - 1:
                            value = outer[r, RAD + sub, place, lanes]
                        else:
                            value = gg[r, 3 * (x - 1) + sub, place, lanes]
                        column.append(value * spread)
                for k, value in enumerate(tent_rows(column)):
                    summed_ref[r, k, place, lanes] = value
            return carry

        lax.fori_loop(0, ext // 8, first_dim, 0)


def force_kernel(nodes_ref, moduli, support, loading, residual_ref):
    cx, cy, _ = support.shape
    lane = lax.broadcasted_iota(jnp.int32, nodes_ref.shape[3:], 1)
    for r in range(3):
        nodes = lambda c, x: nodes_ref[r, c, x]
        for x, sums, below in nodal_rows(nodes, lambda x: moduli[r * cx + x], cx, 0, lane):
            if x < cx:
                free = 1.0 - support[x].astype(jnp.float32)
                for comp in range(3):
                    total = nodal_total(sums, below, comp, lane)[1 : cy + 1]
                    if comp == 2:
                        total = total + load_force * loading[x].astype(jnp.float32)
                    residual_ref[r, comp, x] = -total * free


def final_kernel(
    part, summed, residual, force, support, out_hbm, residual_hbm, compliance_ref, out_ref, row,
    sems,
):
    rows, cols, depth = out_ref.shape
    groups = lane_groups(depth)
    free = 1.0 - support[0].astype(jnp.float32)
    for r in range(3):
        for comp in range(3):
            row[r, comp, 0] = residual[r, comp, 0] - force[r, comp] * free
    copies = [
        pltpu.make_async_copy(residual.at[:, :, 1:], residual_hbm.at[:, :, 1:], sems.at[0]),
        pltpu.make_async_copy(row, residual_hbm.at[:, :, :1], sems.at[1]),
    ]
    for copy in copies:
        copy.start()
    factors = []
    for r in range(3):
        factor = 3.0 * (1.0 - stiff_floor) / 27.0 * sharpness / DENOM[r] ** 3
        factors.append(-factor / part[r : r + 1, :])
    for step in range(rows // 3):
        for sub in range(3):
            k = 3 * step + sub
            parts = []
            for lanes in groups:
                total = None
                for r in range(3):
                    term = factors[r] * summed[r, k, :, lanes]
                    total = term if total is None else total + term
                parts.append(tent_sublanes(total, cols))
            for lanes, value in zip(groups, tent_lanes(parts)):
                out_ref[k, :, lanes] = value
        place = pl.ds(3 * step, 3)
        copies.append(
            pltpu.make_async_copy(out_ref.at[place], out_hbm.at[place], sems.at[2 + step])
        )
        copies[-1].start()
    for r in range(3):
        compliance_ref[r] = jnp.max(part[r : r + 1, :1])
    for copy in copies:
        copy.wait()


def call(kernel, shapes, scratch, flops, args, hbm=0, scalars=(), limit=20, out_hbm=0):
    vmem = pl.BlockSpec(memory_space=pltpu.VMEM)
    smem = pl.BlockSpec(memory_space=pltpu.SMEM)
    scratch = [pltpu.VMEM(s, jnp.float32) if isinstance(s, tuple) else s for s in scratch]
    args = [
        pltpu.with_memory_space_constraint(arg, pltpu.HBM) if i < hbm else arg
        for i, arg in enumerate(args)
    ]
    return pl.pallas_call(
        kernel,
        out_shape=[jax.ShapeDtypeStruct(s, jnp.float32) for s in list(shapes) + list(scalars)],
        in_specs=[pl.BlockSpec(memory_space=pltpu.HBM)] * hbm + [vmem] * (len(args) - hbm),
        out_specs=[pl.BlockSpec(memory_space=pltpu.HBM)] * out_hbm
        + [vmem] * (len(shapes) - out_hbm) + [smem] * len(scalars),
        scratch_shapes=scratch,
        compiler_params=pltpu.CompilerParams(vmem_limit_bytes=limit * 1024 * 1024),
        cost_estimate=pl.CostEstimate(flops=flops, bytes_accessed=1000000, transcendentals=0),
    )(*args)


def ceil8(amount):
    return -(-amount // 8) * 8


def exchange_sum(value, total, group):
    axes = ("wide", "narrow")
    parts = [lax.ppermute(value, axes, [(i, i ^ k) for i in range(total)]) for k in group]
    for part in parts:
        value = value + part
    return value


def local(n_wide, n_narrow, design, passive, displacement, support, loading):
    rows, cols, depth = design.shape
    cx, cy, cz = support.shape
    merged = n_narrow == 2
    axes = ("wide", "narrow")
    ext = ceil8(cols + 2 * RAD)
    padded = ceil8(cy + 3)

    def route(toward, dy):
        pairs = []
        for i in range(n_wide):
            if toward == "down" and i % 2:
                continue
            mate = {"near": i ^ 1, "far": i + 1 if i % 2 else i - 1, "self": i, "down": i - 1}[toward]
            for j in range(n_narrow):
                if 0 <= mate < n_wide and 0 <= j + dy < n_narrow:
                    pairs.append((i * n_narrow + j, mate * n_narrow + j + dy))
        return pairs

    def side_route(toward, index):
        if merged:
            return route(toward, 1) + route(toward, -1)
        return route(toward, 1 if index == 0 else -1)

    def send(block, pairs):
        return lax.ppermute(block, axes, pairs)

    kinds = ("merged",) if merged else ("high", "low")
    sides = len(kinds)
    corner = (ceil8(RAD * REACH + 6), depth)
    ends = (RAD, cols, depth)
    nodes_shape = (3, 3, cx, padded, cz)
    coarse_shape = (3 * cx, padded, cz)
    count = ceil8(cols + 2 * REACH)
    ints = lambda *shape: pltpu.VMEM(shape, jnp.int32)
    packs = call(
        functools.partial(pack_kernel, kinds),
        [(RAD + 1, cols, depth), ends, (3 * cy, depth), nodes_shape]
        + [(ceil8(rows * (REACH + RAD) + 6 * cx), depth), corner] * sides,
        [
            (sides, rows, 8, depth), ints(sides, rows, 8, depth), displacement.shape,
            ints(*support.shape), pltpu.SemaphoreType.DMA((4 + 2 * sides,)),
        ],
        200000, (design, passive, displacement, support), hbm=4,
    )
    far = send(packs[1], route("far", 0))
    got = []
    for index in range(sides):
        side, side_far = packs[4 + 2 * index : 6 + 2 * index]
        side = send(side, side_route("self", index))
        got.append((side, send(side, route("near", 0)), send(side_far, side_route("far", index))))
    near = send(packs[0], route("near", 0))
    row = send(packs[2], route("down", 0))
    own_design, own_mask = call(
        load_kernel, [design.shape, (rows, ext, depth)],
        [ints(*passive.shape), pltpu.SemaphoreType.DMA((2,))],
        200000, (design, passive), hbm=2,
    )
    before, after = got[0], got[-1]
    corners = (before[1], after[1], before[2], after[2])
    outer = (RAD * ext + 3 * padded, depth)
    v, nodes, v_near, v_far = call(
        functools.partial(blur_kernel, n_wide, n_narrow),
        [(rows, ext, depth), nodes_shape, outer, outer],
        [(2,) + ends, (2, 2) + corner, (rows, count, depth), (rows, ext, depth)],
        10000000,
        (own_design, own_mask, packs[3], near, far, before[0], after[0]) + corners,
    )
    v_far = send(v_far, route("far", 0))
    v_near = send(v_near, route("near", 0))
    gg, moduli, part, nodes, energy = call(
        functools.partial(project_kernel, n_wide, n_narrow),
        [
            (3, rows, ext, depth), coarse_shape, (8, LANES), (3, 3, cx + 1, padded, cz),
            coarse_shape,
        ],
        [
            (3 * cx, depth // LANES, ext, LANES), (3 * cx * padded, LANES),
            (3 * cx * padded, LANES), (2,) + corner,
        ],
        10000000, (v, nodes, near, row) + corners,
    )
    total = n_wide * n_narrow
    steps = [1 << bit for bit in range(total.bit_length() - 1)]
    groups = [(s,) for s in steps[:-2]] + [(steps[-2], steps[-1], steps[-2] + steps[-1])]
    (residual,) = call(
        force_kernel, [displacement.shape], [], 10000000,
        (nodes, moduli, support, loading),
    )
    spread_shape = (3 * (cx + 2), depth // LANES, ext, LANES)
    outer_rows, spread, force = call(
        functools.partial(outer_kernel, n_wide, n_narrow),
        [(3, 2 * RAD, ext, depth), spread_shape, (3, 3, cy, cz)],
        [
            (3, 3, 2, padded, cz), (3 * (cx + 2), padded, LANES),
            (RAD, 6, depth // LANES, ext, LANES), (3 * padded, LANES),
        ],
        10000000, (energy, nodes, v_near, v_far),
    )
    (fields,) = call(fields_kernel, [(3, rows, ext, depth)], [], 10000000, (gg, outer_rows, spread))
    summed = part
    for group in groups:
        summed = exchange_sum(summed, total, group)
    sensitivity, residual, compliance = call(
        final_kernel, [design.shape, displacement.shape],
        [design.shape, (3, 3, 1, cy, cz), pltpu.SemaphoreType.DMA((2 + rows // 3,))], 10000000,
        (summed, fields, residual, force, support), scalars=[(3,)], out_hbm=2,
    )
    return residual, compliance, sensitivity


def solution(mesh):
    in_specs = (
        P("wide", "narrow", None),
        P("wide", "narrow", None),
        P(None, None, "wide", "narrow", None),
        P("wide", "narrow", None),
        P("wide", "narrow", None),
    )
    out_specs = (P(None, None, "wide", "narrow", None), P(), P("wide", "narrow", None))

    def body(*args):
        return local(mesh.shape["wide"], mesh.shape["narrow"], *args)

    return jax.shard_map(body, mesh=mesh, in_specs=in_specs, out_specs=out_specs, check_vma=False)
```

```python
import functools
import math

import jax
import jax.numpy as jnp
import numpy as np
from jax import lax
from jax.experimental import pallas as pl
from jax.experimental.pallas import tpu as pltpu
from jax.sharding import PartitionSpec as P


RAD = 3
sharpness = 8.0
thresholds = (0.7, 0.5, 0.3)
stiff_floor = 0.001
load_force = 4.0
poisson = 0.3
LANES = 128
REACH = 2 * RAD
SCALE = 2.0**60


def element_matrix():
    inv_root = 1.0 / np.sqrt(3.0)
    elastic_scale = 1.0 / ((1.0 + poisson) * (1.0 - 2.0 * poisson))
    elastic = np.zeros((6, 6))
    for row_i in range(3):
        for col_j in range(3):
            elastic[row_i, col_j] = poisson
        elastic[row_i, row_i] = 1.0 - poisson
    for row_i in range(3, 6):
        elastic[row_i, row_i] = 0.5 - poisson
    elastic = elastic * elastic_scale
    corner_signs = [
        (2 * (corner // 4) - 1, 2 * (corner // 2 % 2) - 1, 2 * (corner % 2) - 1)
        for corner in range(8)
    ]
    stiffness = np.zeros((24, 24))
    for gauss_a in (-inv_root, inv_root):
        for gauss_b in (-inv_root, inv_root):
            for gauss_c in (-inv_root, inv_root):
                gauss_point = (gauss_a, gauss_b, gauss_c)
                derivs = np.zeros((8, 3))
                for corner in range(8):
                    for along in range(3):
                        slope_value = corner_signs[corner][along] / 8.0
                        for second in range(3):
                            if second != along:
                                slope_value = slope_value * (
                                    1.0 + corner_signs[corner][second] * gauss_point[second]
                                )
                        derivs[corner, along] = 2.0 * slope_value
                strain = np.zeros((6, 24))
                for corner in range(8):
                    column = 3 * corner
                    strain[0, column] = derivs[corner, 0]
                    strain[1, column + 1] = derivs[corner, 1]
                    strain[2, column + 2] = derivs[corner, 2]
                    strain[3, column] = derivs[corner, 1]
                    strain[3, column + 1] = derivs[corner, 0]
                    strain[4, column + 1] = derivs[corner, 2]
                    strain[4, column + 2] = derivs[corner, 1]
                    strain[5, column] = derivs[corner, 2]
                    strain[5, column + 2] = derivs[corner, 0]
                stiffness = stiffness + strain.T @ elastic @ strain * 0.125
    return stiffness


def parity_operator():
    signs = np.ones((8, 8))
    for mode in range(8):
        for corner in range(8):
            for bit in range(3):
                if (mode >> bit) & 1:
                    signs[mode, corner] *= 2 * ((corner >> bit) & 1) - 1
    full = np.kron(signs, np.eye(3))
    coupled = full @ element_matrix() @ full.T / 64.0
    coupled[np.abs(coupled) < 1e-9] = 0.0
    return coupled


COUPLED = parity_operator()
LOW_END = tuple(math.tanh(sharpness * eta) for eta in thresholds)
DENOM = tuple(
    math.tanh(sharpness * eta) + math.tanh(sharpness * (1.0 - eta)) for eta in thresholds
)


def tent_rows(rows):
    for step in (1, 2, 1, 2):
        rows = [rows[i] + rows[i + step] for i in range(len(rows) - step)]
    return rows


def tent_sublanes(block, amount):
    size = block.shape[0]
    for step in (1, 2, 1, 2):
        block = block + pltpu.roll(block, size - step, 0)
    return block[:amount]


def lanes_up(parts, step, lane):
    rolled = [pltpu.roll(part, LANES - step, 1) for part in parts]
    rolled.append(jnp.zeros_like(parts[0]))
    return [
        jnp.where(lane < LANES - step, rolled[g], rolled[g + 1]) for g in range(len(parts))
    ]


def lanes_down(parts, step, lane):
    rolled = [jnp.zeros_like(parts[0])] + [pltpu.roll(part, step, 1) for part in parts]
    return [jnp.where(lane >= step, rolled[g + 1], rolled[g]) for g in range(len(parts))]


def tent_lanes(parts):
    lane = lax.broadcasted_iota(jnp.int32, parts[0].shape, 1)
    total = [4.0 * part for part in parts]
    for step in range(1, RAD + 1):
        ups, downs = lanes_up(parts, step, lane), lanes_down(parts, step, lane)
        if step == RAD:
            total = [t + (u + d) for t, u, d in zip(total, ups, downs)]
        else:
            total = [
                t + float(RAD + 1 - step) * (u + d) for t, u, d in zip(total, ups, downs)
            ]
    return total


def tent_weight(place, extent):
    total = jnp.zeros(place.shape, jnp.float32)
    for offset in range(-RAD, RAD + 1):
        inside = (place + offset >= 0) & (place + offset < extent)
        total = total + jnp.where(inside, float(RAD + 1 - abs(offset)), 0.0)
    return total


def halves(block):
    high = block.astype(jnp.bfloat16)
    low = (block - high.astype(jnp.float32)).astype(jnp.bfloat16)
    return jnp.concatenate([high, low], axis=1)


def lane_groups(depth):
    return [slice(g * LANES, (g + 1) * LANES) for g in range(depth // LANES)]


def modes_of(nodes, row, lane):
    fields = [[[None] * 3 for _ in range(2)] for _ in range(2)]
    for comp in range(3):
        value = nodes(comp, row)
        size = value.shape[0]
        ahead = jnp.where(lane < LANES - 1, pltpu.roll(value, LANES - 1, 1), 0.0)
        for mz, part in enumerate((value + ahead, ahead - value)):
            beside = pltpu.roll(part, size - 1, 0)
            fields[0][mz][comp] = part + beside
            fields[1][mz][comp] = beside - part
    return fields


def element_modes(low, high):
    modes = []
    for mx in range(2):
        for my in range(2):
            for mz in range(2):
                modes.append([
                    (h + l) if mx == 0 else (h - l)
                    for l, h in zip(low[my][mz], high[my][mz])
                ])
    return modes


def coupled_forces(modes):
    forces = [[None] * 3 for _ in range(8)]
    for mode in range(8):
        for comp in range(3):
            row = COUPLED[3 * mode + comp]
            groups = {}
            for place in np.nonzero(row)[0]:
                groups.setdefault(round(float(row[place]), 12), []).append(int(place))
            total = None
            for factor, places in groups.items():
                summed = modes[places[0] // 3][places[0] % 3]
                for place in places[1:]:
                    summed = summed + modes[place // 3][place % 3]
                term = factor * summed
                total = term if total is None else total + term
            forces[mode][comp] = total
    return forces


def pick(n, high, low, kind):
    if kind == "merged":
        return jnp.where(n == 0, high, low)
    return high if kind == "high" else low


def column_start(n, cols, kind):
    if kind == "merged":
        return pl.multiple_of(jnp.where(n == 0, cols - 8, 0), 8)
    return cols - 8 if kind == "high" else 0


def fill_tail(ref, used):
    if ref.shape[0] > used:
        ref[used:, :] = jnp.zeros((ref.shape[0] - used, ref.shape[1]), jnp.float32)


def pack_kernel(
    kinds, design, passive, disp, support, near_ref, far_ref, row_ref, nodes_ref, *rest
):
    rows, cols, depth = design.shape
    cx, cy, _ = support.shape
    sides, (edges, masks, moves, frees, sems) = rest[: 2 * len(kinds)], rest[2 * len(kinds) :]
    groups = lane_groups(depth)
    n = lax.axis_index("narrow")
    even = lax.rem(lax.axis_index("wide"), 2) == 0
    near_start = jnp.where(even, rows - RAD, 0)
    far_start = jnp.where(even, 0, rows - RAD)
    copies = [
        pltpu.make_async_copy(disp, moves, sems.at[0]),
        pltpu.make_async_copy(support, frees, sems.at[1]),
    ]
    for index, kind in enumerate(kinds):
        start = column_start(n, cols, kind)
        copies.append(
            pltpu.make_async_copy(
                design.at[:, pl.ds(start, 8), :], edges.at[index], sems.at[2 + 2 * index]
            )
        )
        copies.append(
            pltpu.make_async_copy(
                passive.at[:, pl.ds(start, 8), :], masks.at[index], sems.at[3 + 2 * index]
            )
        )
    last = 2 + 2 * len(kinds)
    for at, start, ref in ((last, near_start, near_ref), (last + 1, far_start, far_ref)):
        copies.append(
            pltpu.make_async_copy(design.at[pl.ds(start, RAD)], ref.at[:RAD], sems.at[at])
        )
    for copy in copies:
        copy.start()
    nodes_ref[...] = jnp.zeros_like(nodes_ref)
    for copy in copies[:2]:
        copy.wait()
    for x in range(cx):
        free = 1.0 - frees[x].astype(jnp.float32)
        for r in range(3):
            for c in range(3):
                value = moves[r, c, x] * free
                nodes_ref[r, c, x, 1 : cy + 1, :] = value
                if x == 0:
                    near_ref[RAD, r * cy : (r + 1) * cy, groups[c]] = value
                    row_ref[r * cy : (r + 1) * cy, groups[c]] = value
    for copy in copies[2:last]:
        copy.wait()

    for index, kind in enumerate(kinds):
        side, side_far = sides[2 * index : 2 * index + 2]
        for k in range(rows):
            value = edges[index, k]
            piece = pick(n, value[8 - REACH :], value[:REACH], kind)
            side[pl.ds(k * REACH, REACH), :] = piece
            value = 1.0 - masks[index, k].astype(jnp.float32)
            side[pl.ds(rows * REACH + k * RAD, RAD), :] = pick(n, value[8 - RAD :], value[:RAD], kind)
        for k in range(RAD):
            value = edges[index, far_start + k]
            piece = pick(n, value[8 - REACH :], value[:REACH], kind)
            side_far[pl.ds(k * REACH, REACH), :] = piece
        base = rows * (REACH + RAD)
        for r in range(3):
            for c in range(3):
                for x in range(cx):
                    value = nodes_ref[r, c, x]
                    piece = pick(n, value[cy - 1 : cy + 1], value[1:3], kind)
                    side[pl.ds(base + (r * cx + x) * 2, 2), groups[c]] = piece
                    if x == 0:
                        side_far[pl.ds(RAD * REACH + 2 * r, 2), groups[c]] = piece
        fill_tail(side, base + 6 * cx)
        fill_tail(side_far, RAD * REACH + 6)
    for copy in copies[last:]:
        copy.wait()


def element_energy(low, high):
    modes = element_modes(low, high)
    forces = coupled_forces(modes)
    total = None
    for mode in range(8):
        for comp in range(3):
            if forces[mode][comp] is not None:
                term = modes[mode][comp] * forces[mode][comp]
                total = term if total is None else total + term
    return total


def reciprocal_weight(place, extent):
    inside = (place >= 0) & (place < extent)
    return jnp.where(inside, 1.0 / jnp.maximum(tent_weight(place, extent), 1.0), 0.0)


def plane_reciprocals(n, n_narrow, cols, ext, depth):
    place_y = n * cols - RAD + lax.broadcasted_iota(jnp.int32, (ext, LANES), 0)
    recip_y = reciprocal_weight(place_y, n_narrow * cols)
    recip_z = []
    for g in range(depth // LANES):
        place_z = g * LANES + lax.broadcasted_iota(jnp.int32, (ext, LANES), 1)
        recip_z.append(1.0 / tent_weight(place_z, depth))
    return recip_y, recip_z


def low_ends():
    return [jnp.tanh(jnp.full((1, LANES), sharpness * eta, jnp.float32)) for eta in thresholds]


def project_row(row, recip_x, recips, lows, emit, groups):
    recip_y, recip_z = recips
    recip_xy = recip_y * recip_x
    for g, lanes in enumerate(groups):
        recip = recip_xy * recip_z[g]
        scaled = sharpness * row(lanes)
        for r in range(3):
            steep = jnp.tanh(scaled - sharpness * thresholds[r])
            dense = steep + lows[r]
            square = dense * dense
            emit(r, g, lanes, square * (1.0 - steep * steep) * recip, square * dense)


def element_sums(cubes, amount, packed, reach, padded):
    row_id = lax.broadcasted_iota(jnp.int32, (LANES, LANES), 0)
    col_id = lax.broadcasted_iota(jnp.int32, (LANES, LANES), 1)
    total = None
    packed[...] = jnp.zeros_like(packed)
    for g in range(cubes.shape[1]):
        for at in range(amount):
            summed = cubes[at, g, pl.ds(0, reach, stride=3), :]
            summed = summed + cubes[at, g, pl.ds(1, reach, stride=3), :]
            summed = summed + cubes[at, g, pl.ds(2, reach, stride=3), :]
            packed[at * padded : at * padded + reach, :] = summed
        gather = ((g * LANES + row_id) // 3 == col_id).astype(jnp.float32).astype(jnp.bfloat16)
        term = jnp.dot(
            halves(packed[...]),
            jnp.concatenate([gather, gather], axis=0),
            preferred_element_type=jnp.float32,
        )
        total = term if total is None else total + term
    return total


def modulus_of(value, r, keep):
    value = stiff_floor + ((1.0 - stiff_floor) / 27.0 / DENOM[r] ** 3) * value
    return jnp.where(keep, value, 0.0)


def load_kernel(design_hbm, passive_hbm, design, mask_ref, passive, sems):
    rows, cols, depth = design.shape
    copies = [
        pltpu.make_async_copy(passive_hbm, passive, sems.at[0]),
        pltpu.make_async_copy(design_hbm, design, sems.at[1]),
    ]
    for copy in copies:
        copy.start()
    copies[0].wait()
    for k in range(rows):
        mask_ref[k, RAD : RAD + cols, :] = 1.0 - passive[k].astype(jnp.float32)
        mask_ref[k, :RAD, :] = jnp.zeros((RAD, depth), jnp.float32)
        tail = mask_ref.shape[1] - RAD - cols
        mask_ref[k, RAD + cols :, :] = jnp.zeros((tail, depth), jnp.float32)
    copies[1].wait()


def blur_kernel(
    n_wide, n_narrow, design, mask_in, nodes_in, near, far,
    side_b, side_a, near_b, near_a, far_b, far_a,
    v_ref, nodes_ref, near_ref, far_ref, ends, corners, blurred, edge_mask,
):
    rows, cols, depth = design.shape
    cx = nodes_ref.shape[2]
    cy = cols // 3
    groups = lane_groups(depth)
    n = lax.axis_index("narrow")
    w = lax.axis_index("wide")
    valid_b = jnp.where(n > 0, 1.0, 0.0)
    valid_a = jnp.where(n < n_narrow - 1, 1.0, 0.0)
    ext = v_ref.shape[1]

    above = 1 - lax.rem(w, 2)
    for index, ref in ((above, near), (1 - above, far)):
        for k in range(RAD):
            ends[index, k] = ref[k]
    reach = RAD * REACH
    last = (rows - RAD) * REACH
    for which, (one, other) in enumerate(((near_b, far_b), (near_a, far_a))):
        valid = (valid_b, valid_a)[which]
        piece = jnp.where(above == 1, one[:reach], one[last : last + reach])
        corners[which, above, :reach] = piece * valid
        corners[which, 1 - above, :reach] = other[:reach] * valid

    base = rows * (REACH + RAD)
    for r in range(3):
        for c in range(3):
            lanes = groups[c]
            for x in range(cx):
                nodes_ref[r, c, x] = nodes_in[r, c, x]
                at = base + (r * cx + x) * 2
                nodes_ref[r, c, x, 0:1, :] = side_b[at + 1 : at + 2, lanes] * valid_b
                nodes_ref[r, c, x, cy + 1 : cy + 3, :] = side_a[at : at + 2, lanes] * valid_a

    for start in range(0, cols, 8):
        place = slice(start, start + 8)
        for lanes in groups:
            column = [ends[0, k, place, lanes] for k in range(RAD)]
            column += [design[k, place, lanes] for k in range(rows)]
            column += [ends[1, k, place, lanes] for k in range(RAD)]
            for k, value in enumerate(tent_rows(column)):
                blurred[k, REACH + start : REACH + start + 8, lanes] = value
    span = lambda k: slice(k * REACH, (k + 1) * REACH)
    for which, at, side, valid in ((0, 0, side_b, valid_b), (1, REACH + cols, side_a, valid_a)):
        for lanes in groups:
            column = [corners[which, 0, span(k), lanes] for k in range(RAD)]
            column += [side[span(k), lanes] * valid for k in range(rows)]
            column += [corners[which, 1, span(k), lanes] for k in range(RAD)]
            for k, value in enumerate(tent_rows(column)):
                blurred[k, at : at + REACH, lanes] = value
    tail = blurred.shape[1] - cols - 2 * REACH
    if tail:
        blurred[:, cols + 2 * REACH :, :] = jnp.zeros((rows, tail, depth), jnp.float32)

    edge_mask[...] = mask_in[...]
    for k in range(rows):
        at = rows * REACH + k * RAD
        edge_mask[k, 0:RAD, :] = side_b[at : at + RAD, :]
        edge_mask[k, RAD + cols : 2 * RAD + cols, :] = side_a[at : at + RAD, :]

    recip_y, recip_z = plane_reciprocals(n, n_narrow, cols, ext, depth)

    def fine_row(x, carry):
        for sub in range(3):
            k = 3 * x + sub
            parts = tent_lanes([tent_sublanes(blurred[k, :, lanes], ext) for lanes in groups])
            place_x = w * rows + k + jnp.zeros((8, LANES), jnp.int32)
            recip_x = reciprocal_weight(place_x, n_wide * rows)[0:1]
            recip_xy = recip_y * recip_x
            for g, lanes in enumerate(groups):
                v_ref[k, :, lanes] = (recip_xy * recip_z[g]) * parts[g] * edge_mask[k, :, lanes]
        return carry

    for x in range(cx):
        fine_row(x, 0)

    near_first, near_x = above * (rows - RAD), 1 + above * (cx - 2)
    for ref, first, x in (
        (near_ref, near_first, near_x), (far_ref, rows - RAD - near_first, cx - near_x)
    ):
        for k in range(RAD):
            ref[k * ext : (k + 1) * ext, :] = v_ref[first + k]
        for r in range(3):
            at = RAD * ext + r * nodes_ref.shape[3]
            for c in range(3):
                ref[at : at + nodes_ref.shape[3], groups[c]] = nodes_ref[r, c, x]


def project_kernel(
    n_wide, n_narrow, v_ref, nodes_in, near, row, near_b, near_a, far_b, far_a,
    gg_ref, moduli_ref, part_ref, nodes_ref, energy, cubes, packed, agg, corners,
):
    rows, ext, depth = v_ref.shape
    cx = rows // 3
    padded = energy.shape[1]
    groups = lane_groups(depth)
    n = lax.axis_index("narrow")
    w = lax.axis_index("wide")
    cy = (ext - 2 * RAD) // 3
    cols = 3 * cy
    reach = cy + 2

    even = lax.rem(w, 2) == 0
    valid = (jnp.where(n > 0, 1.0, 0.0), jnp.where(n < n_narrow - 1, 1.0, 0.0))
    for which, (one, other) in enumerate(((near_b, far_b), (near_a, far_a))):
        for r in range(3):
            here = rows * (REACH + RAD) + r * cx * 2
            there = RAD * REACH + 2 * r
            piece = jnp.where(even, one[here : here + 2], other[there : there + 2])
            corners[which, 2 * r : 2 * r + 2] = piece * valid[which]
    for r in range(3):
        span = slice(r * cy, (r + 1) * cy)
        at = 2 * r
        for c in range(3):
            lanes = groups[c]
            for x in range(cx):
                nodes_ref[r, c, x] = nodes_in[r, c, x]
            nodes_ref[r, c, cx] = jnp.zeros_like(nodes_ref[r, c, cx])
            nodes_ref[r, c, cx, 1 : cy + 1, :] = jnp.where(even, near[RAD, span, lanes], row[span, lanes])
            nodes_ref[r, c, cx, 0:1, :] = corners[0, at + 1 : at + 2, lanes]
            nodes_ref[r, c, cx, cy + 1 : cy + 3, :] = corners[1, at : at + 2, lanes]
    lane = lax.broadcasted_iota(jnp.int32, nodes_ref.shape[3:], 1)
    for r in range(3):
        nodes = lambda c, x: nodes_ref[r, c, x]
        low = modes_of(nodes, 0, lane)
        for x in range(cx):
            high = modes_of(nodes, x + 1, lane)
            energy[r * cx + x] = element_energy(low, high)
            low = high

    recips = plane_reciprocals(n, n_narrow, cols, ext, depth)
    lows = low_ends()

    def coarse_row(x, carry):
        for sub in range(3):
            k = 3 * x + sub
            place_x = w * rows + k + jnp.zeros((8, LANES), jnp.int32)
            recip_x = reciprocal_weight(place_x, n_wide * rows)[0:1]

            def emit(r, g, lanes, gradient, cube):
                gg_ref[r, k, :, lanes] = gradient
                at = r * cx + x
                cubes[at, g] = cube if sub == 0 else cubes[at, g] + cube

            project_row(lambda lanes: v_ref[k, :, lanes], recip_x, recips, lows, emit, groups)
        return carry

    lax.fori_loop(0, cx, coarse_row, 0)

    agg[...] = element_sums(cubes, 3 * cx, packed, reach, padded)
    sub_id = lax.broadcasted_iota(jnp.int32, (padded, LANES), 0)
    keep = (sub_id > jnp.where(n > 0, -1, 0)) & (sub_id < reach)
    own = ((sub_id >= 1) & (sub_id <= cy)).astype(jnp.float32)
    part_ref[...] = jnp.zeros_like(part_ref)
    for r in range(3):
        partial = None
        for x in range(cx):
            at = r * cx + x
            value = modulus_of(agg[at * padded : (at + 1) * padded, :], r, keep)
            moduli_ref[at] = value
            term = value * energy[at]
            partial = term if partial is None else partial + term
        summed = jnp.sum(jnp.sum(partial * own, axis=0, keepdims=True), axis=1, keepdims=True)
        part_ref[r : r + 1, :] = jnp.broadcast_to(summed, (1, LANES))


def nodal_rows(nodes, moduli, cx, first, lane):
    low = modes_of(nodes, first, lane)
    below = None
    for x in range(first, cx + 1):
        sums, above = None, None
        if x < cx:
            high = modes_of(nodes, x + 1, lane)
            forces = coupled_forces(element_modes(low, high))
            low = high
            modulus = moduli(x)
            scaled = [[None if f is None else modulus * f for f in mode] for mode in forces]
            sums = [[[None] * 3 for _ in range(2)] for _ in range(2)]
            above = [[[None] * 3 for _ in range(2)] for _ in range(2)]
            for my in range(2):
                for mz in range(2):
                    for comp in range(3):
                        even = scaled[2 * my + mz][comp]
                        odd = scaled[4 + 2 * my + mz][comp]
                        sums[my][mz][comp] = -odd if even is None else even - odd
                        above[my][mz][comp] = odd if even is None else even + odd
        yield x, sums, below
        below = above


def nodal_total(sums, below, comp, lane):
    along = []
    for mz in range(2):
        pair = []
        for my in range(2):
            terms = [part[my][mz][comp] for part in (sums, below) if part is not None]
            pair.append(terms[0] if len(terms) == 1 else terms[0] + terms[1])
        along.append((pair[0] - pair[1]) + pltpu.roll(pair[0] + pair[1], 1, 0))
    return (along[0] - along[1]) + jnp.where(
        lane >= 1, pltpu.roll(along[0] + along[1], 1, 1), 0.0
    )


def outer_kernel(
    n_wide, n_narrow, energy, nodes_ref, near, far,
    outer, spread_ref, force_ref, extra_ref, packed, cubes, packed_outer,
):
    _, _, ext, depth = outer.shape
    cx = nodes_ref.shape[2] - 1
    rows = 3 * cx
    cols = 3 * ((ext - 2 * RAD) // 3)
    padded = energy.shape[1]
    reach = ext // 3
    groups = lane_groups(depth)
    n = lax.axis_index("narrow")
    w = lax.axis_index("wide")
    above = 1 - lax.rem(w, 2)
    row_id = lax.broadcasted_iota(jnp.int32, (LANES, LANES), 0)
    col_id = lax.broadcasted_iota(jnp.int32, (LANES, LANES), 1)
    coarse = cx + 2
    lane = lax.broadcasted_iota(jnp.int32, (padded, LANES), 1)
    for r in range(3):
        base = r * coarse
        for x in range(cx):
            packed[base + x + 1] = SCALE * energy[r * cx + x]
        span = slice(RAD * ext + r * padded, RAD * ext + (r + 1) * padded)
        for c in range(3):
            extra_ref[r, c, above] = near[span, groups[c]]
            extra_ref[r, c, 1 - above] = far[span, groups[c]]
        first, last = (
            modes_of(lambda c, x: nodes_ref[r, c, x], x, lane) for x in (0, cx)
        )
        below, beyond = (
            modes_of(lambda c, x: extra_ref[r, c, x], x, lane) for x in (0, 1)
        )
        packed[base] = SCALE * element_energy(below, first)
        packed[base + cx + 1] = SCALE * element_energy(last, beyond)
    split = halves(packed[...].reshape(3 * coarse * padded, LANES))
    for g in range(len(groups)):
        copies = (row_id == (g * LANES + col_id) // 3).astype(jnp.float32).astype(jnp.bfloat16)
        fine = jnp.dot(
            split, jnp.concatenate([copies, copies], axis=0), preferred_element_type=jnp.float32
        )
        for at in range(3 * coarse):
            value = fine[at * padded : at * padded + reach]
            for sub in range(3):
                spread_ref[at, g, pl.ds(sub, reach, stride=3), :] = value
            if 3 * reach < ext:
                spread_ref[at, g, 3 * reach :, :] = jnp.zeros((ext - 3 * reach, LANES), jnp.float32)

    recips = plane_reciprocals(n, n_narrow, cols, ext, depth)
    lows = low_ends()

    def neighbour_row(k, carry):
        at = pl.multiple_of(k * ext, 8)
        for ref, side in ((near, above), (far, 1 - above)):
            first = w * rows + jnp.where(side == 0, -RAD, rows)
            place_x = first + k + jnp.zeros((8, LANES), jnp.int32)
            recip_x = reciprocal_weight(place_x, n_wide * rows)[0:1]

            def emit(r, g, lanes, gradient, cube):
                outer[r, side * RAD + k, :, lanes] = gradient
                cubes[k, side * 3 + r, g] = cube

            project_row(
                lambda lanes: ref[pl.ds(at, ext), lanes], recip_x, recips, lows, emit, groups
            )
        return carry

    lax.fori_loop(0, RAD, neighbour_row, 0)

    for r in range(3):
        for g in range(len(groups)):
            cubes[0, r, g] = cubes[0, r, g] + cubes[1, r, g] + cubes[2, r, g]
    sums = element_sums(cubes.at[0], 3, packed_outer, reach, padded)
    sub_id = lax.broadcasted_iota(jnp.int32, (padded, LANES), 0)
    last = jnp.where(w > 0, reach, 0)
    keep = (sub_id > jnp.where(n > 0, -1, 0)) & (sub_id < last)
    cy = cols // 3
    for r in range(3):
        modulus = modulus_of(sums[r * padded : (r + 1) * padded], r, keep)
        nodes = lambda c, x: extra_ref[r, c, 0] if x < 0 else nodes_ref[r, c, x]
        for x, sums_at, below in nodal_rows(nodes, lambda x: modulus, 0, -1, lane):
            if x == 0:
                for comp in range(3):
                    total = nodal_total(sums_at, below, comp, lane)
                    force_ref[r, comp] = total[1 : cy + 1]


def fields_kernel(gg, outer, spread_ref, summed_ref, rowwise):
    _, rows, ext, depth = gg.shape
    coarse = rows // 3 + 2
    groups = lane_groups(depth)
    for r in range(3):
        def first_dim(s, carry):
            place = pl.ds(pl.multiple_of(8 * s, 8), 8)
            for g, lanes in enumerate(groups):
                column = []
                for x in range(coarse):
                    spread = spread_ref[r * coarse + x, g, place, :]
                    for sub in range(3):
                        if x == 0:
                            value = outer[r, sub, place, lanes]
                        elif x == coarse - 1:
                            value = outer[r, RAD + sub, place, lanes]
                        else:
                            value = gg[r, 3 * (x - 1) + sub, place, lanes]
                        column.append(value * spread)
                for k, value in enumerate(tent_rows(column)):
                    rowwise[k, place, lanes] = value
            return carry

        lax.fori_loop(0, ext // 8, first_dim, 0)

        def second_dim(x, carry):
            for sub in range(3):
                for lanes in groups:
                    value = tent_sublanes(rowwise[3 * x + sub, :, lanes], summed_ref.shape[2])
                    summed_ref[r, 3 * x + sub, :, lanes] = value
            return carry

        lax.fori_loop(0, rows // 3, second_dim, 0)


def force_kernel(nodes_ref, moduli, support, loading, residual_ref):
    cx, cy, _ = support.shape
    lane = lax.broadcasted_iota(jnp.int32, nodes_ref.shape[3:], 1)
    for r in range(3):
        nodes = lambda c, x: nodes_ref[r, c, x]
        for x, sums, below in nodal_rows(nodes, lambda x: moduli[r * cx + x], cx, 0, lane):
            if x < cx:
                free = 1.0 - support[x].astype(jnp.float32)
                for comp in range(3):
                    total = nodal_total(sums, below, comp, lane)[1 : cy + 1]
                    if comp == 2:
                        total = total + load_force * loading[x].astype(jnp.float32)
                    residual_ref[r, comp, x] = -total * free


def final_kernel(
    part, summed, residual, force, support, out_hbm, residual_hbm, compliance_ref, out_ref, row,
    sems,
):
    rows, _, depth = out_ref.shape
    groups = lane_groups(depth)
    free = 1.0 - support[0].astype(jnp.float32)
    for r in range(3):
        for comp in range(3):
            row[r, comp, 0] = residual[r, comp, 0] - force[r, comp] * free
    copies = [
        pltpu.make_async_copy(residual.at[:, :, 1:], residual_hbm.at[:, :, 1:], sems.at[0]),
        pltpu.make_async_copy(row, residual_hbm.at[:, :, :1], sems.at[1]),
    ]
    for copy in copies:
        copy.start()
    factors = []
    for r in range(3):
        factor = 3.0 * (1.0 - stiff_floor) / 27.0 * sharpness / DENOM[r] ** 3
        factors.append((-factor / SCALE) / part[r : r + 1, :])
    for step in range(rows // 3):
        for sub in range(3):
            k = 3 * step + sub
            parts = []
            for lanes in groups:
                total = None
                for r in range(3):
                    term = factors[r] * summed[r, k, :, lanes]
                    total = term if total is None else total + term
                parts.append(total)
            for lanes, value in zip(groups, tent_lanes(parts)):
                out_ref[k, :, lanes] = value
        place = pl.ds(3 * step, 3)
        copies.append(
            pltpu.make_async_copy(out_ref.at[place], out_hbm.at[place], sems.at[2 + step])
        )
        copies[-1].start()
    for r in range(3):
        compliance_ref[r] = jnp.max(part[r : r + 1, :1])
    for copy in copies:
        copy.wait()


def call(kernel, shapes, scratch, flops, args, hbm=0, scalars=(), limit=20, out_hbm=0):
    vmem = pl.BlockSpec(memory_space=pltpu.VMEM)
    smem = pl.BlockSpec(memory_space=pltpu.SMEM)
    scratch = [pltpu.VMEM(s, jnp.float32) if isinstance(s, tuple) else s for s in scratch]
    args = [
        pltpu.with_memory_space_constraint(arg, pltpu.HBM) if i < hbm else arg
        for i, arg in enumerate(args)
    ]
    return pl.pallas_call(
        kernel,
        out_shape=[jax.ShapeDtypeStruct(s, jnp.float32) for s in list(shapes) + list(scalars)],
        in_specs=[pl.BlockSpec(memory_space=pltpu.HBM)] * hbm + [vmem] * (len(args) - hbm),
        out_specs=[pl.BlockSpec(memory_space=pltpu.HBM)] * out_hbm
        + [vmem] * (len(shapes) - out_hbm) + [smem] * len(scalars),
        scratch_shapes=scratch,
        compiler_params=pltpu.CompilerParams(vmem_limit_bytes=limit * 1024 * 1024),
        cost_estimate=pl.CostEstimate(flops=flops, bytes_accessed=1000000, transcendentals=0),
    )(*args)


def ceil8(amount):
    return -(-amount // 8) * 8


def exchange_sum(value, total, group):
    axes = ("wide", "narrow")
    parts = [lax.ppermute(value, axes, [(i, i ^ k) for i in range(total)]) for k in group]
    for part in parts:
        value = value + part
    return value


def local(n_wide, n_narrow, design, passive, displacement, support, loading):
    rows, cols, depth = design.shape
    cx, cy, cz = support.shape
    merged = n_narrow == 2
    axes = ("wide", "narrow")
    ext = ceil8(cols + 2 * RAD)
    padded = ceil8(cy + 3)

    def route(toward, dy):
        pairs = []
        for i in range(n_wide):
            if toward == "down" and i % 2:
                continue
            mate = {"near": i ^ 1, "far": i + 1 if i % 2 else i - 1, "self": i, "down": i - 1}[toward]
            for j in range(n_narrow):
                if 0 <= mate < n_wide and 0 <= j + dy < n_narrow:
                    pairs.append((i * n_narrow + j, mate * n_narrow + j + dy))
        return pairs

    def side_route(toward, index):
        if merged:
            return route(toward, 1) + route(toward, -1)
        return route(toward, 1 if index == 0 else -1)

    def send(block, pairs):
        return lax.ppermute(block, axes, pairs)

    kinds = ("merged",) if merged else ("high", "low")
    sides = len(kinds)
    corner = (ceil8(RAD * REACH + 6), depth)
    ends = (RAD, cols, depth)
    nodes_shape = (3, 3, cx, padded, cz)
    coarse_shape = (3 * cx, padded, cz)
    count = ceil8(cols + 2 * REACH)
    ints = lambda *shape: pltpu.VMEM(shape, jnp.int32)
    packs = call(
        functools.partial(pack_kernel, kinds),
        [(RAD + 1, cols, depth), ends, (3 * cy, depth), nodes_shape]
        + [(ceil8(rows * (REACH + RAD) + 6 * cx), depth), corner] * sides,
        [
            (sides, rows, 8, depth), ints(sides, rows, 8, depth), displacement.shape,
            ints(*support.shape), pltpu.SemaphoreType.DMA((4 + 2 * sides,)),
        ],
        200000, (design, passive, displacement, support), hbm=4,
    )
    far = send(packs[1], route("far", 0))
    got = []
    for index in range(sides):
        side, side_far = packs[4 + 2 * index : 6 + 2 * index]
        side = send(side, side_route("self", index))
        got.append((side, send(side, route("near", 0)), send(side_far, side_route("far", index))))
    near = send(packs[0], route("near", 0))
    row = send(packs[2], route("down", 0))
    own_design, own_mask = call(
        load_kernel, [design.shape, (rows, ext, depth)],
        [ints(*passive.shape), pltpu.SemaphoreType.DMA((2,))],
        200000, (design, passive), hbm=2,
    )
    before, after = got[0], got[-1]
    corners = (before[1], after[1], before[2], after[2])
    outer = (RAD * ext + 3 * padded, depth)
    v, nodes, v_near, v_far = call(
        functools.partial(blur_kernel, n_wide, n_narrow),
        [(rows, ext, depth), nodes_shape, outer, outer],
        [(2,) + ends, (2, 2) + corner, (rows, count, depth), (rows, ext, depth)],
        10000000,
        (own_design, own_mask, packs[3], near, far, before[0], after[0]) + corners,
    )
    v_far = send(v_far, route("far", 0))
    v_near = send(v_near, route("near", 0))
    gg, moduli, part, nodes, energy = call(
        functools.partial(project_kernel, n_wide, n_narrow),
        [
            (3, rows, ext, depth), coarse_shape, (8, LANES), (3, 3, cx + 1, padded, cz),
            coarse_shape,
        ],
        [
            (3 * cx, depth // LANES, ext, LANES), (3 * cx * padded, LANES),
            (3 * cx * padded, LANES), (2,) + corner,
        ],
        10000000, (v, nodes, near, row) + corners,
    )
    total = n_wide * n_narrow
    steps = [1 << bit for bit in range(total.bit_length() - 1)]
    groups = [(s,) for s in steps[:-2]] + [(steps[-2], steps[-1], steps[-2] + steps[-1])]
    (residual,) = call(
        force_kernel, [displacement.shape], [], 10000000,
        (nodes, moduli, support, loading),
    )
    spread_shape = (3 * (cx + 2), depth // LANES, ext, LANES)
    outer_rows, spread, force = call(
        functools.partial(outer_kernel, n_wide, n_narrow),
        [(3, 2 * RAD, ext, depth), spread_shape, (3, 3, cy, cz)],
        [
            (3, 3, 2, padded, cz), (3 * (cx + 2), padded, LANES),
            (RAD, 6, depth // LANES, ext, LANES), (3 * padded, LANES),
        ],
        10000000, (energy, nodes, v_near, v_far),
    )
    (fields,) = call(
        fields_kernel, [(3, rows, cols, depth)], [(rows, ext, depth)], 10000000,
        (gg, outer_rows, spread),
    )
    summed = part
    for group in groups:
        summed = exchange_sum(summed, total, group)
    sensitivity, residual, compliance = call(
        final_kernel, [design.shape, displacement.shape],
        [design.shape, (3, 3, 1, cy, cz), pltpu.SemaphoreType.DMA((2 + rows // 3,))], 10000000,
        (summed, fields, residual, force, support), scalars=[(3,)], out_hbm=2,
    )
    return residual, compliance, sensitivity


def solution(mesh):
    in_specs = (
        P("wide", "narrow", None),
        P("wide", "narrow", None),
        P(None, None, "wide", "narrow", None),
        P("wide", "narrow", None),
        P("wide", "narrow", None),
    )
    out_specs = (P(None, None, "wide", "narrow", None), P(), P("wide", "narrow", None))

    def body(*args):
        return local(mesh.shape["wide"], mesh.shape["narrow"], *args)

    return jax.shard_map(body, mesh=mesh, in_specs=in_specs, out_specs=out_specs, check_vma=False)
```
